8 devices in a mesh: bs: 2 (over z, y), tp: 4 (over x, core).
Axes of the slice: x: 2, y: 2, z: 1, core: 2. Of those that a mesh axis runs over, the one named last changes fastest.
Arguments:
- new_hidden: bfloat16 [512, 2560], P('bs'), parts along dimension 0
- cache_k: bfloat16 [512, 64, 32, 80], P('bs', None, 'tp'), parts along dimension 0
- cache_v: bfloat16 [512, 64, 32, 80], P('bs', None, 'tp'), parts along dimension 0
- lengths: int32 [512], P('bs'), parts along dimension 0
- ln1_gain: float32 [2560], replicated
- ln1_bias: float32 [2560], replicated
- w_q: bfloat16 [2560, 2560], P(None, 'tp')
- w_k: bfloat16 [2560, 2560], P(None, 'tp')
- w_v: bfloat16 [2560, 2560], P(None, 'tp')
- w_o: bfloat16 [2560, 2560], P('tp')
- ln2_gain: float32 [2560], replicated
- ln2_bias: float32 [2560], replicated
- w_up: bfloat16 [2560, 10240], P(None, 'tp')
- w_down: bfloat16 [10240, 2560], P('tp')
- lnf_gain: float32 [2560], replicated
- lnf_bias: float32 [2560], replicated
- w_out: bfloat16 [2560, 51200], P(None, 'tp')
Outputs:
- output 1: float32 [512, 51200], P('bs', 'tp'), parts along dimension 0
- output 2: bfloat16 [512, 64, 32, 80], P('bs', None, 'tp'), parts along dimension 0
- output 3: bfloat16 [512, 64, 32, 80], P('bs', None, 'tp'), parts along dimension 0
- output 4: bfloat16 [512, 2560], P('bs'), parts along dimension 0
There are 2 independent parts. The reference program is written for one: setup_inputs(seed, part) draws one part's arguments, and reference() takes and returns one part's arrays. A program takes and returns all parts, laid end to end along the dimension named above; an argument that names none is the same for every part.
All inputs are finite; a program needn't handle non-finite values.
Results may differ from the reference program's by a relative error of at most 0.0149567.
Values are sent between devices in bfloat16 or wider.
A program may use at most 1 GiB of HBM per device.

```python
import math
import jax
import jax.numpy as jnp
from jax import lax

BATCH = 256
CACHE_LEN = 64
D_MODEL = 2560
HEADS = 32
KV_HEADS = 32
HEAD_DIM = 80
FF_DIM = 10240
VOCAB_SIZE = 51200
TP_SIZE = 4

EPSILON = 1e-5
ROPE_BASE = 10000.0
KV_GROUP = HEADS // KV_HEADS
SCORE_SCALE = HEAD_DIM ** -0.5
KEY_SCALE = math.sqrt(math.log(CACHE_LEN / 16.0) + 1.0)
LEN_BITS = int(math.log2(CACHE_LEN))


def layer_norm1p(values, gain, bias):
    mean = jnp.mean(values, axis=-1, keepdims=True)
    centered = values - mean
    variance = jnp.mean(jnp.square(centered), axis=-1, keepdims=True)
    return centered * lax.rsqrt(variance + EPSILON) * (1.0 + gain) + bias


def apply_rotary(vecs, positions):
    rot_dim = HEAD_DIM // 2
    half_rot = rot_dim // 2
    exponent = -2.0 * jnp.arange(half_rot, dtype=jnp.float32) / rot_dim
    inv_freq = ROPE_BASE ** exponent
    angles = positions.astype(jnp.float32)[:, None] * inv_freq[None, :]
    cosine = jnp.cos(angles)[:, None, :]
    sine = jnp.sin(angles)[:, None, :]
    first = vecs[..., :half_rot]
    second = vecs[..., half_rot:rot_dim]
    return jnp.concatenate([first * cosine - second * sine, second * cosine + first * sine, vecs[..., rot_dim:]], axis=-1)


def split_sum(activations, weight):
    act_blocks = jnp.transpose(activations.reshape(BATCH, TP_SIZE, -1), (1, 0, 2))
    weight_blocks = weight.reshape(TP_SIZE, -1, D_MODEL)

    def block_product(pair):
        return jnp.dot(pair[0], pair[1], preferred_element_type=jnp.float32).astype(jnp.bfloat16)

    partials = lax.map(block_product, (act_blocks, weight_blocks))
    return jnp.sum(partials.astype(jnp.float32), axis=0)


def draw_lengths(key):
    exp_key, off_key, long_key, short_key = jax.random.split(key, 4)
    exponent = jax.random.randint(exp_key, (BATCH,), 0, LEN_BITS)
    low_end = jnp.left_shift(jnp.ones((BATCH,), jnp.int32), exponent)
    offset = jax.random.randint(off_key, (BATCH,), 0, 1 << 30) % low_end
    raw_len = low_end + offset
    long_row = jax.random.randint(long_key, (), 0, BATCH)
    short_row = (long_row + jax.random.randint(short_key, (), 1, BATCH)) % BATCH
    rows = jnp.arange(BATCH)
    picked = jnp.where(rows == long_row, CACHE_LEN - 1, jnp.where(rows == short_row, 1, raw_len))
    return picked.astype(jnp.int32)


def setup_inputs(seed: int = 0, part: int = 0) -> dict:
    root_key = jax.random.key(seed)
    shared_root, group_root = jax.random.split(root_key)
    group_keys = jax.random.split(jax.random.fold_in(group_root, part), 4)
    shared_keys = jax.random.split(shared_root, 13)
    cache_shape = (BATCH, CACHE_LEN, KV_HEADS, HEAD_DIM)

    def gaussian(key, shape, scale):
        return scale * jax.random.normal(key, shape, jnp.float32)

    d_scale = 1.0 / math.sqrt(D_MODEL)
    o_scale = 1.0 / math.sqrt(HEADS * HEAD_DIM)
    ff_scale = 1.0 / math.sqrt(FF_DIM)
    return {
        'new_hidden': gaussian(group_keys[0], (BATCH, D_MODEL), 1.0).astype(jnp.bfloat16),
        'cache_k': gaussian(group_keys[1], cache_shape, KEY_SCALE).astype(jnp.bfloat16),
        'cache_v': gaussian(group_keys[2], cache_shape, 2.0).astype(jnp.bfloat16),
        'lengths': draw_lengths(group_keys[3]),
        'ln1_gain': gaussian(shared_keys[0], (D_MODEL,), 0.4),
        'ln1_bias': gaussian(shared_keys[1], (D_MODEL,), 0.4),
        'w_q': gaussian(shared_keys[2], (D_MODEL, HEADS * HEAD_DIM), d_scale).astype(jnp.bfloat16),
        'w_k': gaussian(shared_keys[3], (D_MODEL, KV_HEADS * HEAD_DIM), KEY_SCALE * d_scale).astype(jnp.bfloat16),
        'w_v': gaussian(shared_keys[4], (D_MODEL, KV_HEADS * HEAD_DIM), 2.0 * d_scale).astype(jnp.bfloat16),
        'w_o': gaussian(shared_keys[5], (HEADS * HEAD_DIM, D_MODEL), o_scale).astype(jnp.bfloat16),
        'ln2_gain': gaussian(shared_keys[6], (D_MODEL,), 0.4),
        'ln2_bias': gaussian(shared_keys[7], (D_MODEL,), 0.4),
        'w_up': gaussian(shared_keys[8], (D_MODEL, FF_DIM), d_scale).astype(jnp.bfloat16),
        'w_down': gaussian(shared_keys[9], (FF_DIM, D_MODEL), ff_scale).astype(jnp.bfloat16),
        'lnf_gain': gaussian(shared_keys[10], (D_MODEL,), 0.4),
        'lnf_bias': gaussian(shared_keys[11], (D_MODEL,), 0.4),
        'w_out': gaussian(shared_keys[12], (D_MODEL, VOCAB_SIZE), 2.0 * d_scale).astype(jnp.bfloat16),
    }


def reference(new_hidden, cache_k, cache_v, lengths, ln1_gain, ln1_bias, w_q, w_k, w_v, w_o, ln2_gain, ln2_bias, w_up, w_down, lnf_gain, lnf_bias, w_out):
    hidden_f = new_hidden.astype(jnp.float32)
    normed = layer_norm1p(hidden_f, ln1_gain, ln1_bias).astype(jnp.bfloat16)
    query = jnp.dot(normed, w_q, preferred_element_type=jnp.float32).reshape(BATCH, HEADS, HEAD_DIM)
    key_new = jnp.dot(normed, w_k, preferred_element_type=jnp.float32).reshape(BATCH, KV_HEADS, HEAD_DIM)
    val_new = jnp.dot(normed, w_v, preferred_element_type=jnp.float32).reshape(BATCH, KV_HEADS, HEAD_DIM)
    query = apply_rotary(query, lengths).astype(jnp.bfloat16)
    key_new = apply_rotary(key_new, lengths).astype(jnp.bfloat16)
    val_new = val_new.astype(jnp.bfloat16)
    write_slot = (jnp.arange(CACHE_LEN)[None, :] == lengths[:, None])[:, :, None, None]
    new_cache_k = jnp.where(write_slot, key_new[:, None], cache_k)
    new_cache_v = jnp.where(write_slot, val_new[:, None], cache_v)

    def one_sequence(seq_parts):
        q_row, k_rows, v_rows, length = seq_parts
        q_groups = q_row.reshape(KV_HEADS, KV_GROUP, HEAD_DIM).astype(jnp.float32)
        scores = jnp.einsum('grk,lgk->grl', q_groups, k_rows.astype(jnp.float32)) * SCORE_SCALE
        valid = jnp.arange(CACHE_LEN) <= length
        scores = jnp.where(valid[None, None, :], scores, -1e30)
        attn_prob = jax.nn.softmax(scores, axis=-1).astype(jnp.bfloat16)
        mixed = jnp.einsum('grl,lgk->grk', attn_prob.astype(jnp.float32), v_rows.astype(jnp.float32))
        return mixed.astype(jnp.bfloat16).reshape(HEADS * HEAD_DIM)

    attended = lax.map(one_sequence, (query, new_cache_k, new_cache_v, lengths))
    mid_hidden = (hidden_f + split_sum(attended, w_o)).astype(jnp.bfloat16)
    normed_mid = layer_norm1p(mid_hidden.astype(jnp.float32), ln2_gain, ln2_bias).astype(jnp.bfloat16)
    up_proj = jnp.dot(normed_mid, w_up, preferred_element_type=jnp.float32)
    activated = jnp.square(jnp.maximum(up_proj, 0.0)).astype(jnp.bfloat16)
    out_hidden = (mid_hidden.astype(jnp.float32) + split_sum(activated, w_down)).astype(jnp.bfloat16)
    normed_out = layer_norm1p(out_hidden.astype(jnp.float32), lnf_gain, lnf_bias).astype(jnp.bfloat16)
    logits = jnp.dot(normed_out, w_out, preferred_element_type=jnp.float32)
    peak = jnp.max(logits, axis=-1, keepdims=True)
    total = jnp.sum(jnp.exp(logits - peak), axis=-1, keepdims=True)
    log_probs = logits - (peak + jnp.log(total))
    return (log_probs, new_cache_k, new_cache_v, out_hidden)
```

```python
import jax
import jax.numpy as jnp
import numpy as np
from jax import lax
from jax.experimental import pallas as pl
from jax.experimental.pallas import tpu as pltpu
from jax.sharding import PartitionSpec as P

EPSILON = 1e-5
ROPE_BASE = 10000.0
AHEAD = 2
VMEM_LIMIT = 66 * 1000 * 1000


def norm_block(values, gain, bias):
    mean = jnp.mean(values, axis=-1, keepdims=True)
    centered = values - mean
    variance = jnp.mean(jnp.square(centered), axis=-1, keepdims=True)
    return centered * lax.rsqrt(variance + EPSILON) * (1.0 + gain) + bias


def attention_kernel(x_ref, len_ref, freq_ref, gain_ref, bias_ref, wq_hbm, wk_hbm, wv_hbm, wo_hbm, kc_hbm, vc_hbm, part_ref, ko_hbm, vo_hbm, kbuf, vbuf, wbuf, wobuf, h_ref, qkv_ref, tmp_ref, attn_ref, s_ref, w_sem, ki_sem, vi_sem, ko_sem, vo_sem):
    heads, cache_len, head_dim, batch = kbuf.shape
    half_rot = head_dim // 4
    weight_copies = [pltpu.make_async_copy(src, wbuf.at[i], w_sem.at[i]) for i, src in enumerate((wq_hbm, wk_hbm, wv_hbm))]

    def k_in(h):
        return pltpu.make_async_copy(kc_hbm.at[:, h], kbuf.at[h], ki_sem.at[h])

    def v_in(h):
        return pltpu.make_async_copy(vc_hbm.at[:, h], vbuf.at[h], vi_sem.at[h])

    def k_out(h):
        return pltpu.make_async_copy(kbuf.at[h], ko_hbm.at[:, h], ko_sem.at[h])

    def v_out(h):
        return pltpu.make_async_copy(vbuf.at[h], vo_hbm.at[:, h], vo_sem.at[h])

    wo_copy = pltpu.make_async_copy(wo_hbm, wobuf, w_sem.at[3])
    for copy in weight_copies:
        copy.start()
    for h in range(AHEAD):
        k_in(h).start()
        v_in(h).start()

    rows = 32

    def norm_rows(i, carry):
        here = pl.ds(pl.multiple_of(i * rows, rows), rows)
        h_ref[here, :] = norm_block(x_ref[here, :].astype(jnp.float32), gain_ref[...], bias_ref[...]).astype(jnp.bfloat16)
        return carry

    lax.fori_loop(0, batch // rows, norm_rows, 0)

    angles = freq_ref[...] * len_ref[...].astype(jnp.float32)
    upper = lax.broadcasted_iota(jnp.int32, angles.shape, 0) < half_rot
    cosine = jnp.cos(angles)
    sine = jnp.where(upper, -jnp.sin(angles), jnp.sin(angles))

    for i in range(3):
        weight_copies[i].wait()
        flat = jnp.dot(h_ref[...], wbuf[i], preferred_element_type=jnp.float32)
        tmp_ref[...] = flat.T
        for h in range(heads):
            base = h * head_dim
            out = pl.ds(h * head_dim, head_dim)
            if i == 2:
                qkv_ref[i, out, :] = tmp_ref[out, :]
            else:
                first = tmp_ref[pl.ds(base, half_rot), :]
                second = tmp_ref[pl.ds(base + half_rot, half_rot), :]
                both = tmp_ref[pl.ds(base, 2 * half_rot), :]
                swapped = jnp.concatenate([second, first], axis=0)
                qkv_ref[i, pl.ds(base, 2 * half_rot), :] = both * cosine + swapped * sine
                rest = pl.ds(base + 2 * half_rot, head_dim - 2 * half_rot)
                qkv_ref[i, rest, :] = tmp_ref[rest, :]
    wo_copy.start()
    scale = head_dim ** -0.5
    lengths = len_ref[...]

    def one_head(h, carry):
        @pl.when(h + AHEAD < heads)
        def _():
            k_in(h + AHEAD).start()
            v_in(h + AHEAD).start()

        here = pl.ds(pl.multiple_of(h * head_dim, head_dim), head_dim)
        query = qkv_ref[0, here, :].astype(jnp.bfloat16).astype(jnp.float32)
        key_new = qkv_ref[1, here, :].astype(jnp.bfloat16)
        val_new = qkv_ref[2, here, :].astype(jnp.bfloat16)
        k_in(h).wait()

        def score_row(l, c):
            old = kbuf[h, l]
            row = jnp.where(jnp.broadcast_to(lengths == l, old.shape), key_new, old)
            kbuf[h, l] = row
            s_ref[pl.ds(l, 1), :] = jnp.sum(row.astype(jnp.float32) * query, axis=0, keepdims=True)
            return c

        lax.fori_loop(0, cache_len, score_row, 0, unroll=4)
        k_out(h).start()
        scores = s_ref[...] * scale
        valid = lax.broadcasted_iota(jnp.int32, scores.shape, 0) <= lengths
        scores = jnp.where(valid, scores, -1e30)
        weights = jnp.exp(scores - jnp.max(scores, axis=0, keepdims=True))
        s_ref[...] = (weights / jnp.sum(weights, axis=0, keepdims=True)).astype(jnp.bfloat16).astype(jnp.float32)
        v_in(h).wait()

        def mix_row(l, acc):
            old = vbuf[h, l]
            row = jnp.where(jnp.broadcast_to(lengths == l, old.shape), val_new, old)
            vbuf[h, l] = row
            return acc + s_ref[pl.ds(l, 1), :] * row.astype(jnp.float32)

        attn_ref[here, :] = lax.fori_loop(0, cache_len, mix_row, jnp.zeros((head_dim, batch), jnp.float32), unroll=4)
        v_out(h).start()
        return carry

    lax.fori_loop(0, heads, one_head, 0)
    attended = attn_ref[...].T.astype(jnp.bfloat16)
    wo_copy.wait()
    wide = 512
    for n in range(0, part_ref.shape[1], wide):
        part_ref[:, n:n + wide] = jnp.dot(attended, wobuf[:, n:n + wide], preferred_element_type=jnp.float32).astype(jnp.bfloat16)
    for h in range(heads):
        k_out(h).wait()
        v_out(h).wait()


def attend(new_hidden, cache_k, cache_v, lengths, ln1_gain, ln1_bias, w_q, w_k, w_v, w_o):
    batch, cache_len, heads, head_dim = cache_k.shape
    width = new_hidden.shape[1]
    flat = heads * head_dim
    rot_dim = head_dim // 2
    exponent = -2.0 * (np.arange(rot_dim) % (rot_dim // 2)) / rot_dim
    freqs = np.broadcast_to((ROPE_BASE ** exponent).astype(np.float32)[:, None], (rot_dim, batch))
    k_view = jnp.transpose(cache_k, (1, 2, 3, 0))
    v_view = jnp.transpose(cache_v, (1, 2, 3, 0))
    vmem = pl.BlockSpec(memory_space=pltpu.VMEM)
    hbm = pl.BlockSpec(memory_space=pl.ANY)
    cache_bytes = 8 * cache_k.size
    partial, k_new, v_new = pl.pallas_call(
        attention_kernel,
        out_shape=(
            jax.ShapeDtypeStruct((batch, width), jnp.bfloat16),
            jax.ShapeDtypeStruct(k_view.shape, jnp.bfloat16),
            jax.ShapeDtypeStruct(v_view.shape, jnp.bfloat16),
        ),
        in_specs=[vmem] * 5 + [hbm] * 6,
        out_specs=(vmem, hbm, hbm),
        scratch_shapes=[
            pltpu.VMEM((heads, cache_len, head_dim, batch), jnp.bfloat16),
            pltpu.VMEM((heads, cache_len, head_dim, batch), jnp.bfloat16),
            pltpu.VMEM((3, width, flat), jnp.bfloat16),
            pltpu.VMEM((flat, width), jnp.bfloat16),
            pltpu.VMEM((batch, width), jnp.bfloat16),
            pltpu.VMEM((3, flat, batch), jnp.float32),
            pltpu.VMEM((flat, batch), jnp.float32),
            pltpu.VMEM((flat, batch), jnp.float32),
            pltpu.VMEM((cache_len, batch), jnp.float32),
            pltpu.SemaphoreType.DMA((4,)),
            pltpu.SemaphoreType.DMA((heads,)),
            pltpu.SemaphoreType.DMA((heads,)),
            pltpu.SemaphoreType.DMA((heads,)),
            pltpu.SemaphoreType.DMA((heads,)),
        ],
        compiler_params=pltpu.CompilerParams(vmem_limit_bytes=VMEM_LIMIT),
        cost_estimate=pl.CostEstimate(flops=8 * batch * width * flat, bytes_accessed=cache_bytes + 8 * width * flat, transcendentals=0),
        name="attend",
    )(new_hidden, lengths[None, :], jnp.asarray(freqs), ln1_gain[None, :], ln1_bias[None, :], w_q, w_k, w_v, w_o, k_view, v_view)
    return partial, jnp.transpose(k_new, (3, 0, 1, 2)), jnp.transpose(v_new, (3, 0, 1, 2))


def reduce_to_all(partial, residual, ways):
    batch, width = partial.shape
    piece = width // ways
    received = lax.all_to_all(partial, 'tp', 1, 0, tiled=True)
    summed = jnp.sum(received.reshape(ways, batch, piece).astype(jnp.float32), axis=0)
    start = lax.axis_index('tp') * piece
    own_resid = lax.dynamic_slice_in_dim(residual, start, piece, axis=1)
    own_sum = (own_resid.astype(jnp.float32) + summed).astype(jnp.bfloat16)
    return lax.all_gather(own_sum, 'tp', axis=1, tiled=True)


def solution(mesh):
    ways = mesh.shape['tp']
    row_spec = P('bs', None)
    cache_spec = P('bs', None, 'tp', None)
    col_split = P(None, 'tp')
    row_split = P('tp', None)
    in_specs = (row_spec, cache_spec, cache_spec, P('bs'), P(), P(), col_split, col_split, col_split, row_split, P(), P(), col_split, row_split, P(), P(), col_split)
    out_specs = (P('bs', 'tp'), cache_spec, cache_spec, row_spec)

    def local_step(new_hidden, cache_k, cache_v, lengths, ln1_gain, ln1_bias, w_q, w_k, w_v, w_o, ln2_gain, ln2_bias, w_up, w_down, lnf_gain, lnf_bias, w_out):
        partial_o, new_cache_k, new_cache_v = attend(new_hidden, cache_k, cache_v, lengths, ln1_gain, ln1_bias, w_q, w_k, w_v, w_o)
        mid_hidden = reduce_to_all(partial_o, new_hidden, ways)
        normed_mid = norm_block(mid_hidden.astype(jnp.float32), ln2_gain, ln2_bias).astype(jnp.bfloat16)
        up_proj = jnp.dot(normed_mid, w_up, preferred_element_type=jnp.float32)
        activated = jnp.square(jnp.maximum(up_proj, 0.0)).astype(jnp.bfloat16)
        partial_m = jnp.dot(activated, w_down, preferred_element_type=jnp.float32).astype(jnp.bfloat16)
        out_hidden = reduce_to_all(partial_m, mid_hidden, ways)
        normed_out = norm_block(out_hidden.astype(jnp.float32), lnf_gain, lnf_bias).astype(jnp.bfloat16)
        logits = jnp.dot(normed_out, w_out, preferred_element_type=jnp.float32)
        local_peak = jnp.max(logits, axis=-1)
        local_total = jnp.sum(jnp.exp(logits - local_peak[:, None]), axis=-1)
        gathered = lax.all_gather(jnp.stack([local_peak, local_total]), 'tp')
        global_peak = jnp.max(gathered[:, 0], axis=0)
        global_total = jnp.sum(gathered[:, 1] * jnp.exp(gathered[:, 0] - global_peak[None, :]), axis=0)
        log_probs = logits - (global_peak + jnp.log(global_total))[:, None]
        return log_probs, new_cache_k, new_cache_v, out_hidden

    return jax.shard_map(local_step, mesh=mesh, in_specs=in_specs, out_specs=out_specs, check_vma=False)
```

```python
import jax
import jax.numpy as jnp
import numpy as np
from jax import lax
from jax.experimental import pallas as pl
from jax.experimental.pallas import tpu as pltpu
from jax.sharding import PartitionSpec as P

EPSILON = 1e-5
ROPE_BASE = 10000.0
AHEAD = 2
WIDE = 512
SLOTS = 18
EARLY = 14
VMEM_LIMIT = 66 * 1000 * 1000


def norm_block(values, gain, bias):
    mean = jnp.mean(values, axis=-1, keepdims=True)
    centered = values - mean
    variance = jnp.mean(jnp.square(centered), axis=-1, keepdims=True)
    return centered * lax.rsqrt(variance + EPSILON) * (1.0 + gain) + bias


def attention_kernel(x_ref, len_ref, freq_ref, gain_ref, bias_ref, wq_hbm, wk_hbm, wv_hbm, wo_hbm, kc_hbm, vc_hbm, part_ref, ko_hbm, vo_hbm, kbuf, vbuf, wbuf, wobuf, h_ref, qkv_ref, tmp_ref, attn_ref, s_ref, w_sem, ki_sem, vi_sem, ko_sem, vo_sem):
    heads, cache_len, head_dim, batch = kbuf.shape
    half_rot = head_dim // 4
    weight_copies = [pltpu.make_async_copy(src, wbuf.at[i], w_sem.at[i]) for i, src in enumerate((wq_hbm, wk_hbm, wv_hbm))]

    def k_in(h):
        return pltpu.make_async_copy(kc_hbm.at[:, h], kbuf.at[h], ki_sem.at[h])

    def v_in(h):
        return pltpu.make_async_copy(vc_hbm.at[:, h], vbuf.at[h], vi_sem.at[h])

    def k_out(h):
        return pltpu.make_async_copy(kbuf.at[h], ko_hbm.at[:, h], ko_sem.at[h])

    def v_out(h):
        return pltpu.make_async_copy(vbuf.at[h], vo_hbm.at[:, h], vo_sem.at[h])

    wo_copy = pltpu.make_async_copy(wo_hbm, wobuf, w_sem.at[3])
    for copy in weight_copies:
        copy.start()
    for h in range(AHEAD):
        k_in(h).start()
        v_in(h).start()

    rows = 32

    def norm_rows(i, carry):
        here = pl.ds(pl.multiple_of(i * rows, rows), rows)
        h_ref[here, :] = norm_block(x_ref[here, :].astype(jnp.float32), gain_ref[...], bias_ref[...]).astype(jnp.bfloat16)
        return carry

    lax.fori_loop(0, batch // rows, norm_rows, 0)

    angles = freq_ref[...] * len_ref[...].astype(jnp.float32)
    upper = lax.broadcasted_iota(jnp.int32, angles.shape, 0) < half_rot
    cosine = jnp.cos(angles)
    sine = jnp.where(upper, -jnp.sin(angles), jnp.sin(angles))

    for i in range(3):
        weight_copies[i].wait()
        flat = jnp.dot(h_ref[...], wbuf[i], preferred_element_type=jnp.float32)
        tmp_ref[...] = flat.T
        for h in range(heads):
            base = h * head_dim
            out = pl.ds(h * head_dim, head_dim)
            if i == 2:
                qkv_ref[i, out, :] = tmp_ref[out, :]
            else:
                first = tmp_ref[pl.ds(base, half_rot), :]
                second = tmp_ref[pl.ds(base + half_rot, half_rot), :]
                both = tmp_ref[pl.ds(base, 2 * half_rot), :]
                swapped = jnp.concatenate([second, first], axis=0)
                qkv_ref[i, pl.ds(base, 2 * half_rot), :] = both * cosine + swapped * sine
                rest = pl.ds(base + 2 * half_rot, head_dim - 2 * half_rot)
                qkv_ref[i, rest, :] = tmp_ref[rest, :]
    wo_copy.start()
    scale = head_dim ** -0.5
    lengths = len_ref[...]

    def one_head(h, carry):
        @pl.when(h + AHEAD < heads)
        def _():
            k_in(h + AHEAD).start()
            v_in(h + AHEAD).start()

        here = pl.ds(pl.multiple_of(h * head_dim, head_dim), head_dim)
        query = qkv_ref[0, here, :].astype(jnp.bfloat16).astype(jnp.float32)
        key_new = qkv_ref[1, here, :].astype(jnp.bfloat16)
        val_new = qkv_ref[2, here, :].astype(jnp.bfloat16)
        k_in(h).wait()

        def score_row(l, c):
            old = kbuf[h, l]
            row = jnp.where(jnp.broadcast_to(lengths == l, old.shape), key_new, old)
            kbuf[h, l] = row
            s_ref[pl.ds(l, 1), :] = jnp.sum(row.astype(jnp.float32) * query, axis=0, keepdims=True)
            return c

        lax.fori_loop(0, cache_len, score_row, 0, unroll=4)
        k_out(h).start()
        scores = s_ref[...] * scale
        valid = lax.broadcasted_iota(jnp.int32, scores.shape, 0) <= lengths
        scores = jnp.where(valid, scores, -1e30)
        weights = jnp.exp(scores - jnp.max(scores, axis=0, keepdims=True))
        s_ref[...] = (weights / jnp.sum(weights, axis=0, keepdims=True)).astype(jnp.bfloat16).astype(jnp.float32)
        v_in(h).wait()

        def mix_row(l, acc):
            old = vbuf[h, l]
            row = jnp.where(jnp.broadcast_to(lengths == l, old.shape), val_new, old)
            vbuf[h, l] = row
            return acc + s_ref[pl.ds(l, 1), :] * row.astype(jnp.float32)

        attn_ref[here, :] = lax.fori_loop(0, cache_len, mix_row, jnp.zeros((head_dim, batch), jnp.float32), unroll=4)
        v_out(h).start()
        return carry

    lax.fori_loop(0, heads, one_head, 0)
    attended = attn_ref[...].T.astype(jnp.bfloat16)
    wo_copy.wait()
    wide = 512
    for n in range(0, part_ref.shape[1], wide):
        part_ref[:, n:n + wide] = jnp.dot(attended, wobuf[:, n:n + wide], preferred_element_type=jnp.float32).astype(jnp.bfloat16)
    for h in range(heads):
        k_out(h).wait()
        v_out(h).wait()


def attend(new_hidden, cache_k, cache_v, lengths, ln1_gain, ln1_bias, w_q, w_k, w_v, w_o):
    batch, cache_len, heads, head_dim = cache_k.shape
    width = new_hidden.shape[1]
    flat = heads * head_dim
    rot_dim = head_dim // 2
    exponent = -2.0 * (np.arange(rot_dim) % (rot_dim // 2)) / rot_dim
    freqs = np.broadcast_to((ROPE_BASE ** exponent).astype(np.float32)[:, None], (rot_dim, batch))
    k_view = jnp.transpose(cache_k, (1, 2, 3, 0))
    v_view = jnp.transpose(cache_v, (1, 2, 3, 0))
    vmem = pl.BlockSpec(memory_space=pltpu.VMEM)
    hbm = pl.BlockSpec(memory_space=pl.ANY)
    cache_bytes = 8 * cache_k.size
    partial, k_new, v_new = pl.pallas_call(
        attention_kernel,
        out_shape=(
            jax.ShapeDtypeStruct((batch, width), jnp.bfloat16),
            jax.ShapeDtypeStruct(k_view.shape, jnp.bfloat16),
            jax.ShapeDtypeStruct(v_view.shape, jnp.bfloat16),
        ),
        in_specs=[vmem] * 5 + [hbm] * 6,
        out_specs=(vmem, hbm, hbm),
        scratch_shapes=[
            pltpu.VMEM((heads, cache_len, head_dim, batch), jnp.bfloat16),
            pltpu.VMEM((heads, cache_len, head_dim, batch), jnp.bfloat16),
            pltpu.VMEM((3, width, flat), jnp.bfloat16),
            pltpu.VMEM((flat, width), jnp.bfloat16),
            pltpu.VMEM((batch, width), jnp.bfloat16),
            pltpu.VMEM((3, flat, batch), jnp.float32),
            pltpu.VMEM((flat, batch), jnp.float32),
            pltpu.VMEM((flat, batch), jnp.float32),
            pltpu.VMEM((cache_len, batch), jnp.float32),
            pltpu.SemaphoreType.DMA((4,)),
            pltpu.SemaphoreType.DMA((heads,)),
            pltpu.SemaphoreType.DMA((heads,)),
            pltpu.SemaphoreType.DMA((heads,)),
            pltpu.SemaphoreType.DMA((heads,)),
        ],
        compiler_params=pltpu.CompilerParams(vmem_limit_bytes=VMEM_LIMIT),
        cost_estimate=pl.CostEstimate(flops=8 * batch * width * flat, bytes_accessed=cache_bytes + 8 * width * flat, transcendentals=0),
        name="attend",
    )(new_hidden, lengths[None, :], jnp.asarray(freqs), ln1_gain[None, :], ln1_bias[None, :], w_q, w_k, w_v, w_o, k_view, v_view)
    return partial, jnp.transpose(k_new, (3, 0, 1, 2)), jnp.transpose(v_new, (3, 0, 1, 2))


def layer_kernel(part_ref, x_hbm, gain2_hbm, bias2_hbm, gainf_hbm, biasf_hbm, up_hbm, down_hbm, out_hbm, y_ref, z_hbm, lse_ref, slots, recv, recv2, h2, act, part2, hf, x1, xrow, norms, zst, peak, total, stats, load_sem, slot_sem, zout_sem, send_sem, rs_sem, ag_sem, rs2_sem, agf_sem, agy_sem, st_sem):
    batch, width = part_ref.shape
    own_rows = x1.shape[0]
    half = 2 * own_rows
    count, _, wide = slots.shape
    n_up = up_hbm.shape[1] // wide
    n_down = down_hbm.shape[1] // wide
    n_out = out_hbm.shape[1] // wide
    first_out = n_up + n_down
    me = lax.axis_index("tp")
    chip = me // 2
    core = lax.rem(me, 2)
    partner = 2 * chip + 1 - core
    cross = 2 * (1 - chip) + core
    diag = 2 * (1 - chip) + 1 - core
    local = pl.ds(pl.multiple_of(half * chip, half), half)
    remote = pl.ds(pl.multiple_of(half * (1 - chip), half), half)

    def rows_of(owner):
        return pl.ds(pl.multiple_of(own_rows * owner, own_rows), own_rows)

    def cols(n):
        return pl.ds(pl.multiple_of(n * wide, wide), wide)

    def push(src, dst, sem, recv_sem, to):
        return pltpu.make_async_remote_copy(src_ref=src, dst_ref=dst, send_sem=sem, recv_sem=recv_sem, device_id={"tp": to}, device_id_type=pl.DeviceIdType.MESH)

    def load_up(n):
        return pltpu.make_async_copy(up_hbm.at[:, cols(n)], slots.at[n], slot_sem.at[n])

    def load_down(n):
        return pltpu.make_async_copy(down_hbm.at[:, cols(n)], slots.at[n_up + n], slot_sem.at[n_up + n])

    def load_out(j):
        slot = lax.rem(j + first_out, count)
        return pltpu.make_async_copy(out_hbm.at[:, cols(j)], slots.at[slot], slot_sem.at[slot])

    small = [pltpu.make_async_copy(x_hbm.at[rows_of(me), :], xrow, load_sem.at[0])]
    for i, src in enumerate((gain2_hbm, bias2_hbm, gainf_hbm, biasf_hbm)):
        small.append(pltpu.make_async_copy(src, norms.at[i], load_sem.at[i + 1]))
    for copy in small:
        copy.start()

    barrier = pltpu.get_barrier_semaphore()
    for other in (partner, cross, diag):
        pl.semaphore_signal(barrier, inc=1, device_id={"tp": other}, device_id_type=pl.DeviceIdType.MESH)
    pl.semaphore_wait(barrier, 3)

    rs = [push(part_ref.at[rows_of(p), :], recv.at[me], send_sem.at[i], rs_sem.at[me], p) for i, p in enumerate((cross, diag, partner))]
    for copy in rs:
        copy.start()
    for n in range(n_up):
        load_up(n).start()
    for n in range(n_down):
        load_down(n).start()
    for j in range(count - first_out):
        load_out(j).start()
    for copy in small:
        copy.wait()

    def arrived(ref, sem, owner):
        pltpu.make_async_copy(ref, ref, sem.at[owner]).wait()

    for p in (partner, cross, diag):
        arrived(recv.at[p], rs_sem, p)
    step = 16

    def mid_rows(i, carry):
        here = pl.ds(pl.multiple_of(i * step, step), step)
        mine = pl.ds(pl.multiple_of(own_rows * me + i * step, step), step)
        summed = part_ref[mine, :].astype(jnp.float32)
        for p in (partner, cross, diag):
            summed = summed + recv[p, here, :].astype(jnp.float32)
        mid = (xrow[here, :].astype(jnp.float32) + summed).astype(jnp.bfloat16)
        x1[here, :] = mid
        h2[mine, :] = norm_block(mid.astype(jnp.float32), norms[0], norms[1]).astype(jnp.bfloat16)
        return carry

    lax.fori_loop(0, own_rows // step, mid_rows, 0)
    own2 = h2.at[rows_of(me), :]
    ag = [push(own2, own2, send_sem.at[3], ag_sem.at[me], cross), push(own2, own2, send_sem.at[4], ag_sem.at[me], partner)]
    for copy in ag:
        copy.start()

    def mlp_up(rows):
        def body(n, carry):
            up = jnp.dot(h2[rows, :], slots[n], preferred_element_type=jnp.float32)
            act[:, cols(n)] = jnp.square(jnp.maximum(up, 0.0)).astype(jnp.bfloat16)
            return carry

        lax.fori_loop(0, n_up, body, 0)

    def down_block(rows, n):
        part2[rows, cols(n)] = jnp.dot(act[...], slots[n_up + n], preferred_element_type=jnp.float32).astype(jnp.bfloat16)

    arrived(h2.at[rows_of(partner), :], ag_sem, partner)
    for n in range(n_up):
        load_up(n).wait()
    mlp_up(local)
    for n in range(n_down):
        load_down(n).wait()

    def down_local(n, carry):
        down_block(local, n)
        return carry

    lax.fori_loop(0, n_down, down_local, 0)
    to_partner = push(part2.at[rows_of(partner), :], recv2.at[me], send_sem.at[5], rs2_sem.at[me], partner)
    to_partner.start()
    arrived(h2.at[rows_of(cross), :], ag_sem, cross)
    relay2 = push(h2.at[rows_of(cross), :], h2.at[rows_of(cross), :], send_sem.at[6], ag_sem.at[cross], partner)
    relay2.start()
    arrived(h2.at[rows_of(diag), :], ag_sem, diag)
    mlp_up(remote)
    for j in range(count - first_out, count - n_down):
        load_out(j).start()

    def down_remote(n, carry):
        down_block(remote, n)
        for i, p in enumerate((cross, diag)):
            push(part2.at[rows_of(p), cols(n)], recv2.at[me, :, cols(n)], send_sem.at[7 + i], rs2_sem.at[me], p).start()
        return carry

    lax.fori_loop(0, n_down, down_remote, 0)
    for j in range(count - n_down, count):
        load_out(j).start()

    for p in (partner, cross, diag):
        arrived(recv2.at[p], rs2_sem, p)

    def out_rows(i, carry):
        here = pl.ds(pl.multiple_of(i * step, step), step)
        mine = pl.ds(pl.multiple_of(own_rows * me + i * step, step), step)
        summed = part2[mine, :].astype(jnp.float32)
        for p in (partner, cross, diag):
            summed = summed + recv2[p, here, :].astype(jnp.float32)
        out = (x1[here, :].astype(jnp.float32) + summed).astype(jnp.bfloat16)
        y_ref[mine, :] = out
        hf[mine, :] = norm_block(out.astype(jnp.float32), norms[2], norms[3]).astype(jnp.bfloat16)
        return carry

    lax.fori_loop(0, own_rows // step, out_rows, 0)
    ownf = hf.at[rows_of(me), :]
    owny = y_ref.at[rows_of(me), :]
    agf = [push(ownf, ownf, send_sem.at[9], agf_sem.at[me], cross), push(ownf, ownf, send_sem.at[10], agf_sem.at[me], partner)]
    agy = [push(owny, owny, send_sem.at[11], agy_sem.at[me], cross), push(owny, owny, send_sem.at[12], agy_sem.at[me], partner)]
    for copy in agf + agy:
        copy.start()

    peak[...] = jnp.full(peak.shape, -jnp.inf, jnp.float32)
    total[...] = jnp.zeros(total.shape, jnp.float32)
    lanes = peak.shape[1]

    def head_block(rows, j, buf):
        z = jnp.dot(hf[rows, :], slots[lax.rem(j + first_out, count)], preferred_element_type=jnp.float32)
        buf[...] = z
        pieces = [z[:, c:c + lanes] for c in range(0, wide, lanes)]
        old = peak[rows, :]
        new = old
        for piece in pieces:
            new = jnp.maximum(new, piece)
        acc = total[rows, :] * jnp.exp(old - new)
        for piece in pieces:
            acc = acc + jnp.exp(piece - new)
        peak[rows, :] = new
        total[rows, :] = acc

    def head_loop(rows, size, lo, hi, before, after):
        def copy_z(j):
            turn = lax.rem(j, 2)
            return pltpu.make_async_copy(zst.at[turn, pl.ds(0, size), :], z_hbm.at[rows, cols(j)], zout_sem.at[turn])

        def body(j, carry):
            before(j)

            @pl.when(j >= lo + 2)
            def _():
                copy_z(j - 2).wait()

            head_block(rows, j, zst.at[lax.rem(j, 2), pl.ds(0, size), :])
            copy_z(j).start()
            after(j)
            return carry

        lax.fori_loop(lo, hi, body, 0)
        for j in range(hi - 2, hi):
            copy_z(j).wait()

    def nothing(j):
        pass

    def next_out(j):
        @pl.when(j + count < n_out)
        def _():
            load_out(j + count).start()

    arrived(hf.at[rows_of(partner), :], agf_sem, partner)
    head_loop(local, half, 0, EARLY, lambda j: load_out(j).wait(), nothing)
    arrived(hf.at[rows_of(cross), :], agf_sem, cross)
    relayf = push(hf.at[rows_of(cross), :], hf.at[rows_of(cross), :], send_sem.at[13], agf_sem.at[cross], partner)
    relayf.start()
    arrived(hf.at[rows_of(diag), :], agf_sem, diag)
    head_loop(remote, half, 0, EARLY, nothing, next_out)
    arrived(y_ref.at[rows_of(cross), :], agy_sem, cross)
    relayy = push(y_ref.at[rows_of(cross), :], y_ref.at[rows_of(cross), :], send_sem.at[14], agy_sem.at[cross], partner)
    relayy.start()
    head_loop(pl.ds(0, batch), batch, EARLY, n_out, lambda j: load_out(j).wait(), next_out)

    top = jnp.max(peak[...], axis=1, keepdims=True)
    bottom = jnp.sum(total[...] * jnp.exp(peak[...] - top), axis=1, keepdims=True)
    stats[me, 0] = jnp.broadcast_to(top, peak.shape).T[0:8]
    stats[me, 1] = jnp.broadcast_to(bottom, peak.shape).T[0:8]
    st = [push(stats.at[me], stats.at[me], send_sem.at[15 + i], st_sem.at[me], p) for i, p in enumerate((cross, diag, partner))]
    for copy in st:
        copy.start()
    for p in (partner, diag):
        arrived(y_ref.at[rows_of(p), :], agy_sem, p)
    for p in (partner, cross, diag):
        arrived(stats.at[p], st_sem, p)
    tops = [stats[i, 0] for i in range(4)]
    whole_top = jnp.maximum(jnp.maximum(tops[0], tops[1]), jnp.maximum(tops[2], tops[3]))
    whole = sum(stats[i, 1] * jnp.exp(tops[i] - whole_top) for i in range(4))
    lse = whole_top + jnp.log(whole)
    lse_ref[...] = jnp.broadcast_to(lse[0:1], (lanes, batch)).T

    for copy in rs + ag + [to_partner, relay2] + agf + agy + [relayf, relayy] + st:
        copy.wait_send()
    for i, p in enumerate((cross, diag)):
        push(part2.at[rows_of(p), :], recv2.at[me], send_sem.at[7 + i], rs2_sem.at[me], p).wait_send()


def finish_layer(partial, new_hidden, ln2_gain, ln2_bias, lnf_gain, lnf_bias, w_up, w_down, w_out):
    batch, width = partial.shape
    own_rows = batch // 4
    vocab = w_out.shape[1]
    vmem = pl.BlockSpec(memory_space=pltpu.VMEM)
    hbm = pl.BlockSpec(memory_space=pl.ANY)
    dma = pltpu.SemaphoreType.DMA
    bf16, f32 = jnp.bfloat16, jnp.float32
    hidden, logits, lse = pl.pallas_call(
        layer_kernel,
        out_shape=(jax.ShapeDtypeStruct((batch, width), bf16), jax.ShapeDtypeStruct((batch, vocab), f32), jax.ShapeDtypeStruct((batch, 128), f32)),
        in_specs=[vmem] + [hbm] * 8,
        out_specs=(vmem, hbm, vmem),
        scratch_shapes=[
            pltpu.VMEM((SLOTS, width, WIDE), bf16),
            pltpu.VMEM((4, own_rows, width), bf16),
            pltpu.VMEM((4, own_rows, width), bf16),
            pltpu.VMEM((batch, width), bf16),
            pltpu.VMEM((2 * own_rows, w_up.shape[1]), bf16),
            pltpu.VMEM((batch, width), bf16),
            pltpu.VMEM((batch, width), bf16),
            pltpu.VMEM((own_rows, width), bf16),
            pltpu.VMEM((own_rows, width), bf16),
            pltpu.VMEM((4, 1, width), f32),
            pltpu.VMEM((2, batch, WIDE), f32),
            pltpu.VMEM((batch, 128), f32),
            pltpu.VMEM((batch, 128), f32),
            pltpu.VMEM((4, 2, 8, batch), f32),
            dma((5,)), dma((SLOTS,)), dma((2,)), dma((18,)), dma((4,)), dma((4,)), dma((4,)), dma((4,)), dma((4,)), dma((4,)),
        ],
        compiler_params=pltpu.CompilerParams(vmem_limit_bytes=VMEM_LIMIT, collective_id=0, has_side_effects=True),
        cost_estimate=pl.CostEstimate(flops=2 * batch * (w_up.size + w_down.size + w_out.size), bytes_accessed=2 * (w_up.size + w_down.size + w_out.size), transcendentals=batch * vocab),
        name="layer",
    )(partial, new_hidden, ln2_gain[None, :], ln2_bias[None, :], lnf_gain[None, :], lnf_bias[None, :], w_up, w_down, w_out)
    return hidden, logits - lse[:, :1]


def solution(mesh):
    row_spec = P('bs', None)
    cache_spec = P('bs', None, 'tp', None)
    col_split = P(None, 'tp')
    row_split = P('tp', None)
    in_specs = (row_spec, cache_spec, cache_spec, P('bs'), P(), P(), col_split, col_split, col_split, row_split, P(), P(), col_split, row_split, P(), P(), col_split)
    out_specs = (P('bs', 'tp'), cache_spec, cache_spec, row_spec)

    def local_step(new_hidden, cache_k, cache_v, lengths, ln1_gain, ln1_bias, w_q, w_k, w_v, w_o, ln2_gain, ln2_bias, w_up, w_down, lnf_gain, lnf_bias, w_out):
        partial_o, new_cache_k, new_cache_v = attend(new_hidden, cache_k, cache_v, lengths, ln1_gain, ln1_bias, w_q, w_k, w_v, w_o)
        out_hidden, log_probs = finish_layer(partial_o, new_hidden, ln2_gain, ln2_bias, lnf_gain, lnf_bias, w_up, w_down, w_out)
        return log_probs, new_cache_k, new_cache_v, out_hidden

    return jax.shard_map(local_step, mesh=mesh, in_specs=in_specs, out_specs=out_specs, check_vma=False)
```

```python
import math
import jax
import jax.numpy as jnp
from jax import lax
from jax.experimental import pallas as pl
from jax.experimental.pallas import tpu as pltpu
from jax.sharding import PartitionSpec as P

EPSILON = 1e-5
ROPE_BASE = 10000.0
AHEAD_FAR = 6
AHEAD_NEAR = 3
WIDE = 512
SLOTS = 18
EARLY = 14
RELAY = 11
VMEM_LIMIT = 66 * 1000 * 1000


def norm_block(values, gain, bias):
    mean = jnp.mean(values, axis=-1, keepdims=True)
    centered = values - mean
    variance = jnp.mean(jnp.square(centered), axis=-1, keepdims=True)
    return centered * lax.rsqrt(variance + EPSILON) * (1.0 + gain) + bias


def attend_lanes(start, ahead, lengths, project, part, kc_hbm, vc_hbm, ko_hbm, vo_hbm, kbuf, vbuf, attn_ref, s_ref, ki_sem, vi_sem, ko_sem, vo_sem):
    heads, cache_len, head_dim, batch = kbuf.shape
    lanes = pl.ds(pl.multiple_of(start, batch), batch)

    def k_in(h):
        return pltpu.make_async_copy(kc_hbm.at[:, h, :, lanes], kbuf.at[h], ki_sem.at[h])

    def v_in(h):
        return pltpu.make_async_copy(vc_hbm.at[:, h, :, lanes], vbuf.at[h], vi_sem.at[h])

    def k_out(h):
        return pltpu.make_async_copy(kbuf.at[h], ko_hbm.at[:, h, :, lanes], ko_sem.at[h])

    def v_out(h):
        return pltpu.make_async_copy(vbuf.at[h], vo_hbm.at[:, h, :, lanes], vo_sem.at[h])

    for h in range(ahead):
        k_in(h).start()
        v_in(h).start()
    qkv = project()
    scale = head_dim ** -0.5

    def one_head(h, carry):
        @pl.when(h + ahead < heads)
        def _():
            k_in(h + ahead).start()
            v_in(h + ahead).start()

        here = pl.ds(pl.multiple_of(h * head_dim, head_dim), head_dim)
        query = qkv[0, here, :].astype(jnp.bfloat16).astype(jnp.float32)
        key_new = qkv[1, here, :].astype(jnp.bfloat16)
        val_new = qkv[2, here, :].astype(jnp.bfloat16)
        k_in(h).wait()

        def score_row(l, c):
            old = kbuf[h, l]
            row = jnp.where(jnp.broadcast_to(lengths == l, old.shape), key_new, old)
            kbuf[h, l] = row
            s_ref[pl.ds(l, 1), :] = jnp.sum(row.astype(jnp.float32) * query, axis=0, keepdims=True)
            return c

        lax.fori_loop(0, cache_len, score_row, 0, unroll=8)
        k_out(h).start()
        scores = s_ref[...] * scale
        valid = lax.broadcasted_iota(jnp.int32, scores.shape, 0) <= lengths
        scores = jnp.where(valid, scores, -1e30)
        weights = jnp.exp(scores - jnp.max(scores, axis=0, keepdims=True))
        s_ref[...] = (weights / jnp.sum(weights, axis=0, keepdims=True)).astype(jnp.bfloat16).astype(jnp.float32)
        v_in(h).wait()

        def mix_row(l, acc):
            old = vbuf[h, l]
            row = jnp.where(jnp.broadcast_to(lengths == l, old.shape), val_new, old)
            vbuf[h, l] = row
            return acc + s_ref[pl.ds(l, 1), :] * row.astype(jnp.float32)

        attn_ref[here, :] = lax.fori_loop(0, cache_len, mix_row, jnp.zeros((head_dim, batch), jnp.float32), unroll=8)
        v_out(h).start()
        return carry

    lax.fori_loop(0, heads, one_head, 0)
    part(attn_ref[...].T.astype(jnp.bfloat16))
    for h in range(heads):
        k_out(h).wait()
        v_out(h).wait()


def far_kernel(x_ref, len_ref, gain_ref, bias_ref, wq_hbm, wk_hbm, wv_hbm, wo_hbm, kc_hbm, vc_hbm, cross_ref, diag_ref, near_ref, ko_hbm, vo_hbm, kbuf, vbuf, wbuf, wobuf, h_ref, qkv_ref, tmp_ref, attn_ref, s_ref, far_ref, w_sem, ki_sem, vi_sem, ko_sem, vo_sem):
    heads, cache_len, head_dim, half = kbuf.shape
    batch = x_ref.shape[0]
    half_rot = head_dim // 4
    me = lax.axis_index("tp")
    chip = me // 2
    core = lax.rem(me, 2)
    copies = [pltpu.make_async_copy(src, wbuf.at[i], w_sem.at[i]) for i, src in enumerate((wq_hbm, wk_hbm, wv_hbm))]
    wo_copy = pltpu.make_async_copy(wo_hbm, wobuf, w_sem.at[3])
    for copy in copies:
        copy.start()
    rows = 32
    gain, bias = gain_ref[...][None, :], bias_ref[...][None, :]

    def project():
        def norm_rows(i, carry):
            here = pl.ds(pl.multiple_of(i * rows, rows), rows)
            h_ref[here, :] = norm_block(x_ref[here, :].astype(jnp.float32), gain, bias).astype(jnp.bfloat16)
            return carry

        lax.fori_loop(0, batch // rows, norm_rows, 0)
        index = lax.broadcasted_iota(jnp.int32, (2 * half_rot, batch), 0)
        upper = index < half_rot
        pair = jnp.where(upper, index, index - half_rot).astype(jnp.float32)
        angles = jnp.exp(pair * (-math.log(ROPE_BASE) / half_rot)) * len_ref[...].astype(jnp.float32)
        cosine = jnp.cos(angles)
        sine = jnp.where(upper, -jnp.sin(angles), jnp.sin(angles))
        for i in range(3):
            copies[i].wait()
            tmp_ref[...] = jnp.dot(h_ref[...], wbuf[i], preferred_element_type=jnp.float32).T
            for h in range(heads):
                base = h * head_dim
                if i == 2:
                    blocks = [(base, head_dim, tmp_ref[pl.ds(base, head_dim), :])]
                else:
                    first = tmp_ref[pl.ds(base, half_rot), :]
                    second = tmp_ref[pl.ds(base + half_rot, half_rot), :]
                    both = tmp_ref[pl.ds(base, 2 * half_rot), :]
                    swapped = jnp.concatenate([second, first], axis=0)
                    rest = head_dim - 2 * half_rot
                    blocks = [(base, 2 * half_rot, both * cosine + swapped * sine), (base + 2 * half_rot, rest, tmp_ref[pl.ds(base + 2 * half_rot, rest), :])]
                for at, size, value in blocks:
                    qkv_ref[0, i, pl.ds(at, size), :] = value[:, :half]
                    qkv_ref[1, i, pl.ds(at, size), :] = value[:, half:]
        wo_copy.start()
        near_ref[...] = qkv_ref[chip]
        return qkv_ref.at[1 - chip]

    def part(attended):
        wo_copy.wait()
        wide = 512
        for n in range(0, far_ref.shape[1], wide):
            far_ref[:, n:n + wide] = jnp.dot(attended, wobuf[:, n:n + wide], preferred_element_type=jnp.float32).astype(jnp.bfloat16)
        own = half // 2
        cross_ref[...] = far_ref[pl.ds(pl.multiple_of(own * core, own), own), :]
        diag_ref[...] = far_ref[pl.ds(pl.multiple_of(own * (1 - core), own), own), :]

    start = half * (1 - chip)
    lengths = len_ref[:, pl.ds(pl.multiple_of(start, half), half)]
    attend_lanes(start, AHEAD_FAR, lengths, project, part, kc_hbm, vc_hbm, ko_hbm, vo_hbm, kbuf, vbuf, attn_ref, s_ref, ki_sem, vi_sem, ko_sem, vo_sem)


def near_kernel(len_ref, qkv_ref, wo_hbm, kc_hbm, vc_hbm, ko_in, vo_in, part_ref, ko_hbm, vo_hbm, kbuf, vbuf, wobuf, attn_ref, s_ref, w_sem, ki_sem, vi_sem, ko_sem, vo_sem):
    half = kbuf.shape[3]
    chip = lax.axis_index("tp") // 2
    start = half * chip
    lengths = len_ref[:, pl.ds(pl.multiple_of(start, half), half)]
    wo_copy = pltpu.make_async_copy(wo_hbm, wobuf, w_sem.at[0])

    def project():
        wo_copy.start()
        return qkv_ref

    def part(attended):
        wo_copy.wait()
        wide = 512
        for n in range(0, part_ref.shape[1], wide):
            part_ref[:, n:n + wide] = jnp.dot(attended, wobuf[:, n:n + wide], preferred_element_type=jnp.float32).astype(jnp.bfloat16)

    attend_lanes(start, AHEAD_NEAR, lengths, project, part, kc_hbm, vc_hbm, ko_hbm, vo_hbm, kbuf, vbuf, attn_ref, s_ref, ki_sem, vi_sem, ko_sem, vo_sem)


def attend(new_hidden, cache_k, cache_v, lengths, ln1_gain, ln1_bias, w_q, w_k, w_v, w_o):
    batch, cache_len, heads, head_dim = cache_k.shape
    width = new_hidden.shape[1]
    flat = heads * head_dim
    half = batch // 2
    k_view = jnp.transpose(cache_k, (1, 2, 3, 0))
    v_view = jnp.transpose(cache_v, (1, 2, 3, 0))
    vmem = pl.BlockSpec(memory_space=pltpu.VMEM)
    hbm = pl.BlockSpec(memory_space=pl.ANY)
    dma = pltpu.SemaphoreType.DMA
    bf16, f32 = jnp.bfloat16, jnp.float32
    shape = jax.ShapeDtypeStruct
    lens = lengths[None, :]
    slabs = [pltpu.VMEM((heads, cache_len, head_dim, half), bf16)] * 2
    sems = [dma((heads,))] * 4
    to_cross, to_diag, near, k_half, v_half = pl.pallas_call(
        far_kernel,
        out_shape=(shape((half // 2, width), bf16), shape((half // 2, width), bf16), shape((3, flat, half), f32), shape(k_view.shape, bf16), shape(v_view.shape, bf16)),
        in_specs=[vmem] * 4 + [hbm] * 6,
        out_specs=(vmem, vmem, vmem, hbm, hbm),
        scratch_shapes=slabs + [
            pltpu.VMEM((3, width, flat), bf16),
            pltpu.VMEM((flat, width), bf16),
            pltpu.VMEM((batch, width), bf16),
            pltpu.VMEM((2, 3, flat, half), f32),
            pltpu.VMEM((flat, batch), f32),
            pltpu.VMEM((flat, half), f32),
            pltpu.VMEM((cache_len, half), f32),
            pltpu.VMEM((half, width), bf16),
            dma((4,)),
        ] + sems,
        compiler_params=pltpu.CompilerParams(vmem_limit_bytes=VMEM_LIMIT),
        cost_estimate=pl.CostEstimate(flops=8 * batch * width * flat, bytes_accessed=4 * cache_k.size + 8 * width * flat, transcendentals=0),
        name="far",
    )(new_hidden, lens, ln1_gain, ln1_bias, w_q, w_k, w_v, w_o, k_view, v_view)
    from_cross = lax.ppermute(to_cross, "tp", [(i, (i + 2) % 4) for i in range(4)])
    from_diag = lax.ppermute(to_diag, "tp", [(i, 3 - i) for i in range(4)])
    partial, k_new, v_new = pl.pallas_call(
        near_kernel,
        out_shape=(shape((half, width), bf16), shape(k_view.shape, bf16), shape(v_view.shape, bf16)),
        in_specs=[vmem] * 2 + [hbm] * 5,
        out_specs=(vmem, hbm, hbm),
        input_output_aliases={5: 1, 6: 2},
        scratch_shapes=slabs + [
            pltpu.VMEM((flat, width), bf16),
            pltpu.VMEM((flat, half), f32),
            pltpu.VMEM((cache_len, half), f32),
            dma((1,)),
        ] + sems,
        compiler_params=pltpu.CompilerParams(vmem_limit_bytes=VMEM_LIMIT),
        cost_estimate=pl.CostEstimate(flops=40 * batch * width * flat, bytes_accessed=4 * cache_k.size, transcendentals=0),
        name="near",
    )(lens, near, w_o, k_view, v_view, k_half, v_half)
    return (partial, from_cross, from_diag), jnp.transpose(k_new, (3, 0, 1, 2)), jnp.transpose(v_new, (3, 0, 1, 2))


def layer_kernel(near_ref, cross_ref, diag_ref, x_hbm, gain2_hbm, bias2_hbm, gainf_hbm, biasf_hbm, up_hbm, down_hbm, out_hbm, y_ref, z_hbm, lse_ref, slots, recv, recv2, h2, act, part2, hf, x1, xrow, norms, zst, peak, total, stats, load_sem, slot_sem, zout_sem, send_sem, rs_sem, ag_sem, rs2_sem, agf_sem, agy_sem, st_sem):
    batch, width = y_ref.shape
    own_rows = x1.shape[0]
    half = 2 * own_rows
    count, _, wide = slots.shape
    n_up = up_hbm.shape[1] // wide
    n_down = down_hbm.shape[1] // wide
    n_out = out_hbm.shape[1] // wide
    first_out = n_up + n_down
    me = lax.axis_index("tp")
    chip = me // 2
    core = lax.rem(me, 2)
    partner = 2 * chip + 1 - core
    cross = 2 * (1 - chip) + core
    diag = 2 * (1 - chip) + 1 - core
    local = pl.ds(pl.multiple_of(half * chip, half), half)
    remote = pl.ds(pl.multiple_of(half * (1 - chip), half), half)

    def rows_of(owner):
        return pl.ds(pl.multiple_of(own_rows * owner, own_rows), own_rows)

    def cols(n):
        return pl.ds(pl.multiple_of(n * wide, wide), wide)

    def push(src, dst, sem, recv_sem, to):
        return pltpu.make_async_remote_copy(src_ref=src, dst_ref=dst, send_sem=sem, recv_sem=recv_sem, device_id={"tp": to}, device_id_type=pl.DeviceIdType.MESH)

    def load_up(n):
        return pltpu.make_async_copy(up_hbm.at[:, cols(n)], slots.at[n], slot_sem.at[n])

    def load_down(n):
        return pltpu.make_async_copy(down_hbm.at[:, cols(n)], slots.at[n_up + n], slot_sem.at[n_up + n])

    def load_out(j):
        slot = lax.rem(j + first_out, count)
        return pltpu.make_async_copy(out_hbm.at[:, cols(j)], slots.at[slot], slot_sem.at[slot])

    small = [pltpu.make_async_copy(x_hbm.at[rows_of(me), :], xrow, load_sem.at[0])]
    for i, src in enumerate((gain2_hbm, bias2_hbm, gainf_hbm, biasf_hbm)):
        small.append(pltpu.make_async_copy(src, norms.at[i], load_sem.at[i + 1]))
    for copy in small:
        copy.start()

    barrier = pltpu.get_barrier_semaphore()
    for other in (partner, cross, diag):
        pl.semaphore_signal(barrier, inc=1, device_id={"tp": other}, device_id_type=pl.DeviceIdType.MESH)
    pl.semaphore_wait(barrier, 3)

    rs = [push(near_ref.at[rows_of(1 - core), :], recv, send_sem.at[0], rs_sem.at[0], partner)]
    for copy in rs:
        copy.start()
    for n in range(n_up):
        load_up(n).start()
    for n in range(n_down):
        load_down(n).start()
    for j in range(count - first_out):
        load_out(j).start()
    for copy in small:
        copy.wait()

    def arrived(ref, sem, owner):
        pltpu.make_async_copy(ref, ref, sem.at[owner]).wait()

    arrived(recv, rs_sem, 0)
    step = 16

    def mid_rows(i, carry):
        here = pl.ds(pl.multiple_of(i * step, step), step)
        mine = pl.ds(pl.multiple_of(own_rows * me + i * step, step), step)
        summed = near_ref[pl.ds(pl.multiple_of(own_rows * core + i * step, step), step), :].astype(jnp.float32)
        for other in (recv, cross_ref, diag_ref):
            summed = summed + other[here, :].astype(jnp.float32)
        mid = (xrow[here, :].astype(jnp.float32) + summed).astype(jnp.bfloat16)
        x1[here, :] = mid
        h2[mine, :] = norm_block(mid.astype(jnp.float32), norms[0][None, :], norms[1][None, :]).astype(jnp.bfloat16)
        return carry

    lax.fori_loop(0, own_rows // step, mid_rows, 0)
    own2 = h2.at[rows_of(me), :]
    ag = [push(own2, own2, send_sem.at[3], ag_sem.at[me], cross), push(own2, own2, send_sem.at[4], ag_sem.at[me], partner)]
    for copy in ag:
        copy.start()

    def mlp_up(rows):
        def body(n, carry):
            up = jnp.dot(h2[rows, :], slots[n], preferred_element_type=jnp.float32)
            act[:, cols(n)] = jnp.square(jnp.maximum(up, 0.0)).astype(jnp.bfloat16)
            return carry

        lax.fori_loop(0, n_up, body, 0)

    def down_block(rows, n):
        part2[rows, cols(n)] = jnp.dot(act[...], slots[n_up + n], preferred_element_type=jnp.float32).astype(jnp.bfloat16)

    arrived(h2.at[rows_of(partner), :], ag_sem, partner)
    for n in range(n_up):
        load_up(n).wait()
    mlp_up(local)
    for n in range(n_down):
        load_down(n).wait()

    def down_local(n, carry):
        down_block(local, n)
        return carry

    lax.fori_loop(0, n_down, down_local, 0)
    to_partner = push(part2.at[rows_of(partner), :], recv2.at[me], send_sem.at[5], rs2_sem.at[me], partner)
    to_partner.start()
    arrived(h2.at[rows_of(cross), :], ag_sem, cross)
    relay2 = push(h2.at[rows_of(cross), :], h2.at[rows_of(cross), :], send_sem.at[6], ag_sem.at[cross], partner)
    relay2.start()
    arrived(h2.at[rows_of(diag), :], ag_sem, diag)
    mlp_up(remote)
    for j in range(count - first_out, count - n_down):
        load_out(j).start()

    def down_remote(n, carry):
        down_block(remote, n)
        for i, p in enumerate((cross, diag)):
            push(part2.at[rows_of(p), cols(n)], recv2.at[me, :, cols(n)], send_sem.at[7 + i], rs2_sem.at[me], p).start()
        return carry

    lax.fori_loop(0, n_down, down_remote, 0)
    for j in range(count - n_down, count):
        load_out(j).start()

    for p in (partner, cross, diag):
        arrived(recv2.at[p], rs2_sem, p)

    def out_rows(i, carry):
        here = pl.ds(pl.multiple_of(i * step, step), step)
        mine = pl.ds(pl.multiple_of(own_rows * me + i * step, step), step)
        summed = part2[mine, :].astype(jnp.float32)
        for p in (partner, cross, diag):
            summed = summed + recv2[p, here, :].astype(jnp.float32)
        out = (x1[here, :].astype(jnp.float32) + summed).astype(jnp.bfloat16)
        y_ref[mine, :] = out
        hf[mine, :] = norm_block(out.astype(jnp.float32), norms[2][None, :], norms[3][None, :]).astype(jnp.bfloat16)
        return carry

    lax.fori_loop(0, own_rows // step, out_rows, 0)
    ownf = hf.at[rows_of(me), :]
    owny = y_ref.at[rows_of(me), :]
    agf = [push(ownf, ownf, send_sem.at[9], agf_sem.at[me], cross), push(ownf, ownf, send_sem.at[10], agf_sem.at[me], partner)]
    agy = [push(owny, owny, send_sem.at[11], agy_sem.at[me], cross), push(owny, owny, send_sem.at[12], agy_sem.at[me], partner)]
    for copy in agf + agy:
        copy.start()

    peak[...] = jnp.full(peak.shape, -jnp.inf, jnp.float32)
    total[...] = jnp.zeros(total.shape, jnp.float32)
    lanes = peak.shape[1]

    def head_dot(rows, j, buf):
        buf[...] = jnp.dot(hf[rows, :], slots[lax.rem(j + first_out, count)], preferred_element_type=jnp.float32)

    def head_stats(rows, buf):
        old = peak[rows, :]
        new = old
        for c in range(0, wide, lanes):
            new = jnp.maximum(new, buf[:, c:c + lanes])
        acc = total[rows, :] * jnp.exp(old - new)
        for c in range(0, wide, lanes):
            acc = acc + jnp.exp(buf[:, c:c + lanes] - new)
        peak[rows, :] = new
        total[rows, :] = acc

    def head_loop(rows, size, lo, hi, before, after):
        def stage(j):
            return zst.at[lax.rem(j, 2), pl.ds(0, size), :]

        def copy_z(j):
            return pltpu.make_async_copy(stage(j), z_hbm.at[rows, cols(j)], zout_sem.at[lax.rem(j, 2)])

        before(lo)
        head_dot(rows, lo, stage(lo))
        copy_z(lo).start()
        after(lo)

        def body(j, carry):
            before(j)

            @pl.when(j >= lo + 2)
            def _():
                copy_z(j - 2).wait()

            head_stats(rows, stage(j - 1))
            head_dot(rows, j, stage(j))
            copy_z(j).start()
            after(j)
            return carry

        lax.fori_loop(lo + 1, hi, body, 0)
        head_stats(rows, stage(hi - 1))
        for j in range(hi - 2, hi):
            copy_z(j).wait()

    def nothing(j):
        pass

    def next_out(j):
        @pl.when(j + count < n_out)
        def _():
            load_out(j + count).start()

    arrived(hf.at[rows_of(partner), :], agf_sem, partner)
    head_loop(local, half, 0, RELAY, lambda j: load_out(j).wait(), nothing)
    arrived(hf.at[rows_of(cross), :], agf_sem, cross)
    relayf = push(hf.at[rows_of(cross), :], hf.at[rows_of(cross), :], send_sem.at[13], agf_sem.at[cross], partner)
    relayf.start()
    head_loop(local, half, RELAY, EARLY, lambda j: load_out(j).wait(), nothing)
    arrived(hf.at[rows_of(diag), :], agf_sem, diag)
    head_loop(remote, half, 0, EARLY, nothing, next_out)
    arrived(y_ref.at[rows_of(cross), :], agy_sem, cross)
    relayy = push(y_ref.at[rows_of(cross), :], y_ref.at[rows_of(cross), :], send_sem.at[14], agy_sem.at[cross], partner)
    relayy.start()
    head_loop(pl.ds(0, batch), batch, EARLY, n_out, lambda j: load_out(j).wait(), next_out)

    top = jnp.max(peak[...], axis=1, keepdims=True)
    bottom = jnp.sum(total[...] * jnp.exp(peak[...] - top), axis=1, keepdims=True)
    stats[me, 0] = jnp.broadcast_to(top, peak.shape).T[0:8]
    stats[me, 1] = jnp.broadcast_to(bottom, peak.shape).T[0:8]
    st = [push(stats.at[me], stats.at[me], send_sem.at[15 + i], st_sem.at[me], p) for i, p in enumerate((cross, diag, partner))]
    for copy in st:
        copy.start()
    for p in (partner, diag):
        arrived(y_ref.at[rows_of(p), :], agy_sem, p)
    for p in (partner, cross, diag):
        arrived(stats.at[p], st_sem, p)
    tops = [stats[i, 0] for i in range(4)]
    whole_top = jnp.maximum(jnp.maximum(tops[0], tops[1]), jnp.maximum(tops[2], tops[3]))
    whole = sum(stats[i, 1] * jnp.exp(tops[i] - whole_top) for i in range(4))
    lse = whole_top + jnp.log(whole)
    lse_ref[...] = jnp.broadcast_to(lse[0:1], (lanes, batch)).T

    for copy in rs + ag + [to_partner, relay2] + agf + agy + [relayf, relayy] + st:
        copy.wait_send()
    for i, p in enumerate((cross, diag)):
        push(part2.at[rows_of(p), :], recv2.at[me], send_sem.at[7 + i], rs2_sem.at[me], p).wait_send()


def subtract_kernel(hidden_ref, lse_ref, logits_hbm, y_ref, logp_hbm, buf, in_sem, out_sem):
    blocks, rows, _ = buf.shape
    ins = [pltpu.make_async_copy(logits_hbm.at[pl.ds(rows * i, rows), :], buf.at[i], in_sem.at[i]) for i in range(blocks)]
    outs = [pltpu.make_async_copy(buf.at[i], logp_hbm.at[pl.ds(rows * i, rows), :], out_sem.at[i]) for i in range(blocks)]
    for copy in ins:
        copy.start()
    y_ref[...] = hidden_ref[...]
    for i in range(blocks):
        ins[i].wait()
        buf[i] = buf[i] - lse_ref[rows * i:rows * (i + 1), 0:1]
        outs[i].start()
    for copy in outs:
        copy.wait()


def finish_layer(partials, new_hidden, ln2_gain, ln2_bias, lnf_gain, lnf_bias, w_up, w_down, w_out):
    batch, width = new_hidden.shape
    own_rows = batch // 4
    vocab = w_out.shape[1]
    vmem = pl.BlockSpec(memory_space=pltpu.VMEM)
    hbm = pl.BlockSpec(memory_space=pl.ANY)
    dma = pltpu.SemaphoreType.DMA
    bf16, f32 = jnp.bfloat16, jnp.float32
    hidden, logits, lse = pl.pallas_call(
        layer_kernel,
        out_shape=(jax.ShapeDtypeStruct((batch, width), bf16), jax.ShapeDtypeStruct((batch, vocab), f32), jax.ShapeDtypeStruct((batch, 128), f32)),
        in_specs=[vmem] * 3 + [hbm] * 8,
        out_specs=(vmem, hbm, vmem),
        scratch_shapes=[
            pltpu.VMEM((SLOTS, width, WIDE), bf16),
            pltpu.VMEM((own_rows, width), bf16),
            pltpu.VMEM((4, own_rows, width), bf16),
            pltpu.VMEM((batch, width), bf16),
            pltpu.VMEM((2 * own_rows, w_up.shape[1]), bf16),
            pltpu.VMEM((batch, width), bf16),
            pltpu.VMEM((batch, width), bf16),
            pltpu.VMEM((own_rows, width), bf16),
            pltpu.VMEM((own_rows, width), bf16),
            pltpu.VMEM((4, width), f32),
            pltpu.VMEM((2, batch, WIDE), f32),
            pltpu.VMEM((batch, 128), f32),
            pltpu.VMEM((batch, 128), f32),
            pltpu.VMEM((4, 2, 8, batch), f32),
            dma((5,)), dma((SLOTS,)), dma((2,)), dma((18,)), dma((1,)), dma((4,)), dma((4,)), dma((4,)), dma((4,)), dma((4,)),
        ],
        compiler_params=pltpu.CompilerParams(vmem_limit_bytes=VMEM_LIMIT, collective_id=0, has_side_effects=True),
        cost_estimate=pl.CostEstimate(flops=2 * batch * (w_up.size + w_down.size + w_out.size), bytes_accessed=2 * (w_up.size + w_down.size + w_out.size), transcendentals=batch * vocab),
        name="layer",
    )(*partials, new_hidden, ln2_gain, ln2_bias, lnf_gain, lnf_bias, w_up, w_down, w_out)
    blocks = 16
    return pl.pallas_call(
        subtract_kernel,
        out_shape=(jax.ShapeDtypeStruct((batch, width), bf16), jax.ShapeDtypeStruct((batch, vocab), f32)),
        in_specs=[vmem, vmem, hbm],
        out_specs=(vmem, hbm),
        scratch_shapes=[pltpu.VMEM((blocks, batch // blocks, vocab), f32), dma((blocks,)), dma((blocks,))],
        compiler_params=pltpu.CompilerParams(vmem_limit_bytes=VMEM_LIMIT),
        cost_estimate=pl.CostEstimate(flops=batch * vocab, bytes_accessed=8 * batch * vocab, transcendentals=0),
        name="subtract",
    )(hidden, lse, logits)


def solution(mesh):
    row_spec = P('bs', None)
    cache_spec = P('bs', None, 'tp', None)
    col_split = P(None, 'tp')
    row_split = P('tp', None)
    in_specs = (row_spec, cache_spec, cache_spec, P('bs'), P(), P(), col_split, col_split, col_split, row_split, P(), P(), col_split, row_split, P(), P(), col_split)
    out_specs = (P('bs', 'tp'), cache_spec, cache_spec, row_spec)

    def local_step(new_hidden, cache_k, cache_v, lengths, ln1_gain, ln1_bias, w_q, w_k, w_v, w_o, ln2_gain, ln2_bias, w_up, w_down, lnf_gain, lnf_bias, w_out):
        partials, new_cache_k, new_cache_v = attend(new_hidden, cache_k, cache_v, lengths, ln1_gain, ln1_bias, w_q, w_k, w_v, w_o)
        out_hidden, log_probs = finish_layer(partials, new_hidden, ln2_gain, ln2_bias, lnf_gain, lnf_bias, w_up, w_down, w_out)
        return log_probs, new_cache_k, new_cache_v, out_hidden

    return jax.shard_map(local_step, mesh=mesh, in_specs=in_specs, out_specs=out_specs, check_vma=False)
```

```python
import math
import jax
import jax.numpy as jnp
from jax import lax
from jax.experimental import pallas as pl
from jax.experimental.pallas import tpu as pltpu
from jax.sharding import PartitionSpec as P

EPSILON = 1e-5
ROPE_BASE = 10000.0
AHEAD_FAR = 6
AHEAD_NEAR = 5
WIDE = 512
SLOTS = 18
GROUP = 5
EARLY = 3
VMEM_LIMIT = 66 * 1000 * 1000


def norm_block(values, gain, bias):
    mean = jnp.mean(values, axis=-1, keepdims=True)
    centered = values - mean
    variance = jnp.mean(jnp.square(centered), axis=-1, keepdims=True)
    return centered * lax.rsqrt(variance + EPSILON) * (1.0 + gain) + bias


def attend_lanes(start, ahead, lengths, project, part, kc_hbm, vc_hbm, ko_hbm, vo_hbm, kbuf, vbuf, attn_ref, s_ref, ki_sem, vi_sem, ko_sem, vo_sem):
    heads, cache_len, head_dim, batch = kbuf.shape
    lanes = pl.ds(pl.multiple_of(start, batch), batch)

    def k_in(h):
        return pltpu.make_async_copy(kc_hbm.at[:, h, :, lanes], kbuf.at[h], ki_sem.at[h])

    def v_in(h):
        return pltpu.make_async_copy(vc_hbm.at[:, h, :, lanes], vbuf.at[h], vi_sem.at[h])

    def k_out(h):
        return pltpu.make_async_copy(kbuf.at[h], ko_hbm.at[:, h, :, lanes], ko_sem.at[h])

    def v_out(h):
        return pltpu.make_async_copy(vbuf.at[h], vo_hbm.at[:, h, :, lanes], vo_sem.at[h])

    for h in range(ahead):
        k_in(h).start()
        v_in(h).start()
    qkv = project()
    scale = head_dim ** -0.5

    def one_head(h, carry):
        @pl.when(h + ahead < heads)
        def _():
            k_in(h + ahead).start()
            v_in(h + ahead).start()

        here = pl.ds(pl.multiple_of(h * head_dim, head_dim), head_dim)
        query = qkv[0, here, :].astype(jnp.bfloat16).astype(jnp.float32)
        key_new = qkv[1, here, :].astype(jnp.bfloat16)
        val_new = qkv[2, here, :].astype(jnp.bfloat16)
        k_in(h).wait()

        def score_row(l, c):
            old = kbuf[h, l]
            row = jnp.where(jnp.broadcast_to(lengths == l, old.shape), key_new, old)
            kbuf[h, l] = row
            s_ref[pl.ds(l, 1), :] = jnp.sum(row.astype(jnp.float32) * query, axis=0, keepdims=True)
            return c

        lax.fori_loop(0, cache_len, score_row, 0, unroll=8)
        k_out(h).start()
        scores = s_ref[...] * scale
        valid = lax.broadcasted_iota(jnp.int32, scores.shape, 0) <= lengths
        scores = jnp.where(valid, scores, -1e30)
        weights = jnp.exp(scores - jnp.max(scores, axis=0, keepdims=True))
        s_ref[...] = (weights / jnp.sum(weights, axis=0, keepdims=True)).astype(jnp.bfloat16).astype(jnp.float32)
        v_in(h).wait()

        def mix_row(l, acc):
            old = vbuf[h, l]
            row = jnp.where(jnp.broadcast_to(lengths == l, old.shape), val_new, old)
            vbuf[h, l] = row
            return acc + s_ref[pl.ds(l, 1), :] * row.astype(jnp.float32)

        attn_ref[here, :] = lax.fori_loop(0, cache_len, mix_row, jnp.zeros((head_dim, batch), jnp.float32), unroll=8)
        v_out(h).start()
        return carry

    lax.fori_loop(0, heads, one_head, 0)
    part(attn_ref[...].T.astype(jnp.bfloat16))
    for h in range(heads):
        k_out(h).wait()
        v_out(h).wait()


def far_kernel(x_ref, len_ref, gain_ref, bias_ref, wq_hbm, wk_hbm, wv_hbm, wo_hbm, kc_hbm, vc_hbm, cross_ref, diag_ref, near_ref, own_ref, ko_hbm, vo_hbm, kbuf, vbuf, wbuf, wobuf, h_ref, qkv_ref, tmp_ref, attn_ref, s_ref, far_ref, w_sem, ki_sem, vi_sem, ko_sem, vo_sem):
    heads, cache_len, head_dim, half = kbuf.shape
    batch = x_ref.shape[0]
    half_rot = head_dim // 4
    me = lax.axis_index("tp")
    chip = me // 2
    core = lax.rem(me, 2)
    copies = [pltpu.make_async_copy(src, wbuf.at[i], w_sem.at[i]) for i, src in enumerate((wq_hbm, wk_hbm, wv_hbm))]
    wo_copy = pltpu.make_async_copy(wo_hbm, wobuf, w_sem.at[3])
    for copy in copies:
        copy.start()
    own_rows = half // 2
    own_ref[...] = x_ref[pl.ds(pl.multiple_of(own_rows * me, own_rows), own_rows), :]
    rows = 32
    gain, bias = gain_ref[...][None, :], bias_ref[...][None, :]

    def project():
        def norm_rows(i, carry):
            here = pl.ds(pl.multiple_of(i * rows, rows), rows)
            h_ref[here, :] = norm_block(x_ref[here, :].astype(jnp.float32), gain, bias).astype(jnp.bfloat16)
            return carry

        lax.fori_loop(0, batch // rows, norm_rows, 0)
        index = lax.broadcasted_iota(jnp.int32, (2 * half_rot, batch), 0)
        upper = index < half_rot
        pair = jnp.where(upper, index, index - half_rot).astype(jnp.float32)
        angles = jnp.exp(pair * (-math.log(ROPE_BASE) / half_rot)) * len_ref[...].astype(jnp.float32)
        cosine = jnp.cos(angles)
        sine = jnp.where(upper, -jnp.sin(angles), jnp.sin(angles))
        for i in range(3):
            copies[i].wait()
            tmp_ref[...] = jnp.dot(h_ref[...], wbuf[i], preferred_element_type=jnp.float32).T
            for h in range(heads):
                base = h * head_dim
                if i == 2:
                    blocks = [(base, head_dim, tmp_ref[pl.ds(base, head_dim), :])]
                else:
                    first = tmp_ref[pl.ds(base, half_rot), :]
                    second = tmp_ref[pl.ds(base + half_rot, half_rot), :]
                    both = tmp_ref[pl.ds(base, 2 * half_rot), :]
                    swapped = jnp.concatenate([second, first], axis=0)
                    rest = head_dim - 2 * half_rot
                    blocks = [(base, 2 * half_rot, both * cosine + swapped * sine), (base + 2 * half_rot, rest, tmp_ref[pl.ds(base + 2 * half_rot, rest), :])]
                for at, size, value in blocks:
                    qkv_ref[0, i, pl.ds(at, size), :] = value[:, :half]
                    qkv_ref[1, i, pl.ds(at, size), :] = value[:, half:]
        wo_copy.start()
        near_ref[...] = qkv_ref[chip]
        return qkv_ref.at[1 - chip]

    def part(attended):
        wo_copy.wait()
        wide = 512
        for n in range(0, far_ref.shape[1], wide):
            far_ref[:, n:n + wide] = jnp.dot(attended, wobuf[:, n:n + wide], preferred_element_type=jnp.float32).astype(jnp.bfloat16)
        own = half // 2
        cross_ref[...] = far_ref[pl.ds(pl.multiple_of(own * core, own), own), :]
        diag_ref[...] = far_ref[pl.ds(pl.multiple_of(own * (1 - core), own), own), :]

    start = half * (1 - chip)
    lengths = len_ref[:, pl.ds(pl.multiple_of(start, half), half)]
    attend_lanes(start, AHEAD_FAR, lengths, project, part, kc_hbm, vc_hbm, ko_hbm, vo_hbm, kbuf, vbuf, attn_ref, s_ref, ki_sem, vi_sem, ko_sem, vo_sem)


def near_kernel(len_ref, qkv_ref, wo_hbm, kc_hbm, vc_hbm, ko_in, vo_in, part_ref, ko_hbm, vo_hbm, kbuf, vbuf, wobuf, attn_ref, s_ref, w_sem, ki_sem, vi_sem, ko_sem, vo_sem):
    half = kbuf.shape[3]
    chip = lax.axis_index("tp") // 2
    start = half * chip
    lengths = len_ref[:, pl.ds(pl.multiple_of(start, half), half)]
    wo_copy = pltpu.make_async_copy(wo_hbm, wobuf, w_sem.at[0])

    def project():
        wo_copy.start()
        return qkv_ref

    def part(attended):
        wo_copy.wait()
        wide = 512
        for n in range(0, part_ref.shape[1], wide):
            part_ref[:, n:n + wide] = jnp.dot(attended, wobuf[:, n:n + wide], preferred_element_type=jnp.float32).astype(jnp.bfloat16)

    attend_lanes(start, AHEAD_NEAR, lengths, project, part, kc_hbm, vc_hbm, ko_hbm, vo_hbm, kbuf, vbuf, attn_ref, s_ref, ki_sem, vi_sem, ko_sem, vo_sem)


def attend(new_hidden, cache_k, cache_v, lengths, ln1_gain, ln1_bias, w_q, w_k, w_v, w_o):
    batch, cache_len, heads, head_dim = cache_k.shape
    width = new_hidden.shape[1]
    flat = heads * head_dim
    half = batch // 2
    k_view = jnp.transpose(cache_k, (1, 2, 3, 0))
    v_view = jnp.transpose(cache_v, (1, 2, 3, 0))
    vmem = pl.BlockSpec(memory_space=pltpu.VMEM)
    hbm = pl.BlockSpec(memory_space=pl.ANY)
    dma = pltpu.SemaphoreType.DMA
    bf16, f32 = jnp.bfloat16, jnp.float32
    shape = jax.ShapeDtypeStruct
    lens = lengths[None, :]
    slabs = [pltpu.VMEM((heads, cache_len, head_dim, half), bf16)] * 2
    sems = [dma((heads,))] * 4
    to_cross, to_diag, near, own, k_half, v_half = pl.pallas_call(
        far_kernel,
        out_shape=(shape((half // 2, width), bf16), shape((half // 2, width), bf16), shape((3, flat, half), f32), shape((half // 2, width), bf16), shape(k_view.shape, bf16), shape(v_view.shape, bf16)),
        in_specs=[vmem] * 4 + [hbm] * 6,
        out_specs=(vmem, vmem, vmem, vmem, hbm, hbm),
        scratch_shapes=slabs + [
            pltpu.VMEM((3, width, flat), bf16),
            pltpu.VMEM((flat, width), bf16),
            pltpu.VMEM((batch, width), bf16),
            pltpu.VMEM((2, 3, flat, half), f32),
            pltpu.VMEM((flat, batch), f32),
            pltpu.VMEM((flat, half), f32),
            pltpu.VMEM((cache_len, half), f32),
            pltpu.VMEM((half, width), bf16),
            dma((4,)),
        ] + sems,
        compiler_params=pltpu.CompilerParams(vmem_limit_bytes=VMEM_LIMIT),
        cost_estimate=pl.CostEstimate(flops=8 * batch * width * flat, bytes_accessed=4 * cache_k.size + 8 * width * flat, transcendentals=0),
        name="far",
    )(new_hidden, lens, ln1_gain, ln1_bias, w_q, w_k, w_v, w_o, k_view, v_view)
    from_cross = lax.ppermute(to_cross, "tp", [(i, (i + 2) % 4) for i in range(4)])
    from_diag = lax.ppermute(to_diag, "tp", [(i, 3 - i) for i in range(4)])
    partial, k_new, v_new = pl.pallas_call(
        near_kernel,
        out_shape=(shape((half, width), bf16), shape(k_view.shape, bf16), shape(v_view.shape, bf16)),
        in_specs=[vmem] * 2 + [hbm] * 5,
        out_specs=(vmem, hbm, hbm),
        input_output_aliases={5: 1, 6: 2},
        scratch_shapes=slabs + [
            pltpu.VMEM((flat, width), bf16),
            pltpu.VMEM((flat, half), f32),
            pltpu.VMEM((cache_len, half), f32),
            dma((1,)),
        ] + sems,
        compiler_params=pltpu.CompilerParams(vmem_limit_bytes=VMEM_LIMIT),
        cost_estimate=pl.CostEstimate(flops=40 * batch * width * flat, bytes_accessed=4 * cache_k.size, transcendentals=0),
        name="near",
    )(lens, near, w_o, k_view, v_view, k_half, v_half)
    return (partial, from_cross, from_diag, own), jnp.transpose(k_new, (3, 0, 1, 2)), jnp.transpose(v_new, (3, 0, 1, 2))


def layer_kernel(near_ref, cross_ref, diag_ref, xrow, gain2_ref, bias2_ref, gainf_ref, biasf_ref, up_hbm, down_hbm, out_hbm, y_hbm, z_hbm, lse_ref, y_ref, slots, recv, recv2, h2, act, act_far, part2, hf, x1, zst, peak, total, stats, load_sem, slot_sem, zout_sem, send_sem, rs_sem, ag_sem, rs2_sem, agf_sem, agy_sem, st_sem):
    batch, width = y_ref.shape
    own_rows = x1.shape[0]
    half = 2 * own_rows
    sub = own_rows // 2
    count, _, wide = slots.shape
    n_up = up_hbm.shape[1] // wide
    n_down = down_hbm.shape[1] // wide
    n_out = out_hbm.shape[1] // wide
    first_out = n_up + n_down
    me = lax.axis_index("tp")
    chip = me // 2
    core = lax.rem(me, 2)
    partner = 2 * chip + 1 - core
    cross = 2 * (1 - chip) + core
    diag = 2 * (1 - chip) + 1 - core
    local = pl.ds(pl.multiple_of(half * chip, half), half)
    remote = pl.ds(pl.multiple_of(half * (1 - chip), half), half)

    def rows_of(owner):
        return pl.ds(pl.multiple_of(own_rows * owner, own_rows), own_rows)

    def cols(n):
        return pl.ds(pl.multiple_of(n * wide, wide), wide)

    def push(src, dst, sem, recv_sem, to):
        return pltpu.make_async_remote_copy(src_ref=src, dst_ref=dst, send_sem=sem, recv_sem=recv_sem, device_id={"tp": to}, device_id_type=pl.DeviceIdType.MESH)

    def load_up(n):
        return pltpu.make_async_copy(up_hbm.at[:, cols(n)], slots.at[n], slot_sem.at[n])

    def load_down(n):
        return pltpu.make_async_copy(down_hbm.at[:, cols(n)], slots.at[n_up + n], slot_sem.at[n_up + n])

    def load_out(j):
        slot = lax.rem(j + first_out, count)
        return pltpu.make_async_copy(out_hbm.at[:, cols(j)], slots.at[slot], slot_sem.at[slot])

    def half_of(owner, s):
        return pl.ds(pl.multiple_of(own_rows * owner + sub * s, sub), sub)

    barrier = pltpu.get_barrier_semaphore()
    for other in (partner, cross, diag):
        pl.semaphore_signal(barrier, inc=1, device_id={"tp": other}, device_id_type=pl.DeviceIdType.MESH)
    for n in range(n_up):
        load_up(n).start()
    for n in range(n_down):
        load_down(n).start()
    pl.semaphore_wait(barrier, 3)

    rs = push(near_ref.at[rows_of(1 - core), :], recv, send_sem.at[0], rs_sem.at[0], partner)
    rs.start()

    def arrived(ref, sem, index):
        pltpu.make_async_copy(ref, ref, sem.at[index]).wait()

    def share(ref, sem, s, first_send):
        rows = ref.at[half_of(me, s), :]
        to_cross = push(rows, rows, send_sem.at[first_send], sem.at[2 * me + s], cross)
        to_partner = push(rows, rows, send_sem.at[first_send + 1], sem.at[2 * me + s], partner)
        to_cross.start()
        to_partner.start()
        return [to_cross, to_partner]

    def relay(ref, sem, s, first_send):
        rows = ref.at[half_of(cross, s), :]
        arrived(rows, sem, 2 * cross + s)
        copy = push(rows, rows, send_sem.at[first_send], sem.at[2 * cross + s], partner)
        copy.start()
        return [copy]

    sent = [rs]
    gain2, bias2 = gain2_ref[...][None, :], bias2_ref[...][None, :]
    arrived(recv, rs_sem, 0)
    for s in range(2):
        here = pl.ds(sub * s, sub)
        summed = near_ref[half_of(core, s), :].astype(jnp.float32)
        for other in (recv, cross_ref, diag_ref):
            summed = summed + other[here, :].astype(jnp.float32)
        mid = (xrow[here, :].astype(jnp.float32) + summed).astype(jnp.bfloat16)
        x1[here, :] = mid
        h2[half_of(me, s), :] = norm_block(mid.astype(jnp.float32), gain2, bias2).astype(jnp.bfloat16)
        sent += share(h2, ag_sem, s, 1 + 2 * s)

    def far_rows(ref, s, columns):
        return jnp.concatenate([ref[half_of(2 * (1 - chip), s), columns], ref[half_of(2 * (1 - chip) + 1, s), columns]], axis=0)

    def squared(up):
        return jnp.square(jnp.maximum(up, 0.0)).astype(jnp.bfloat16)

    def up_near():
        for n in range(n_up):
            act[:, wide * n:wide * (n + 1)] = squared(jnp.dot(h2[local, :], slots[n], preferred_element_type=jnp.float32))

    def up_far(s):
        for n in range(n_up):
            act_far[:, wide * n:wide * (n + 1)] = squared(jnp.dot(far_rows(h2, s, slice(None)), slots[n], preferred_element_type=jnp.float32))

    def down_near():
        for n in range(n_down):
            part2[local, wide * n:wide * (n + 1)] = jnp.dot(act[...], slots[n_up + n], preferred_element_type=jnp.float32).astype(jnp.bfloat16)

    def send_far(p, i, s, n):
        return push(part2.at[half_of(p, s), cols(n)], recv2.at[me, pl.ds(sub * s, sub), cols(n)], send_sem.at[5 + 2 * i + s], rs2_sem.at[2 * me + s], p)

    def down_far(s):
        for lo, hi in ((0, 2), (2, n_down)):
            for n in range(lo, hi):
                down = jnp.dot(act_far[...], slots[n_up + n], preferred_element_type=jnp.float32).astype(jnp.bfloat16)
                part2[half_of(2 * (1 - chip), s), wide * n:wide * (n + 1)] = down[:sub]
                part2[half_of(2 * (1 - chip) + 1, s), wide * n:wide * (n + 1)] = down[sub:]
            for n in range(lo, hi):
                for i, p in enumerate((cross, diag)):
                    send_far(p, i, s, n).start()

    for s in range(2):
        arrived(h2.at[half_of(partner, s), :], ag_sem, 2 * partner + s)
    for n in range(n_up):
        load_up(n).wait()
    for j in range(count - first_out):
        load_out(j).start()
    up_near()
    sent += relay(h2, ag_sem, 0, 9)
    arrived(h2.at[half_of(diag, 0), :], ag_sem, 2 * diag)
    up_far(0)
    sent += relay(h2, ag_sem, 1, 10)
    for n in range(n_down):
        load_down(n).wait()
    down_far(0)
    arrived(h2.at[half_of(diag, 1), :], ag_sem, 2 * diag + 1)
    up_far(1)
    for j in range(count - first_out, count - n_down):
        load_out(j).start()
    down_far(1)
    down_near()
    for j in range(count - n_down, count):
        load_out(j).start()
    for s in range(2):
        copy = push(part2.at[half_of(partner, s), :], recv2.at[me, pl.ds(sub * s, sub), :], send_sem.at[11 + s], rs2_sem.at[2 * me + s], partner)
        copy.start()
        sent.append(copy)

    gainf, biasf = gainf_ref[...][None, :], biasf_ref[...][None, :]
    for s in range(2):
        here = pl.ds(sub * s, sub)
        for p in (partner, cross, diag):
            arrived(recv2.at[p, here, :], rs2_sem, 2 * p + s)
        summed = part2[half_of(me, s), :].astype(jnp.float32)
        for p in (partner, cross, diag):
            summed = summed + recv2[p, here, :].astype(jnp.float32)
        out = (x1[here, :].astype(jnp.float32) + summed).astype(jnp.bfloat16)
        y_ref[half_of(me, s), :] = out
        hf[half_of(me, s), :] = norm_block(out.astype(jnp.float32), gainf, biasf).astype(jnp.bfloat16)
        sent += share(hf, agf_sem, s, 13 + 2 * s)
    owny = y_ref.at[rows_of(me), :]
    for i, p in enumerate((cross, partner)):
        copy = push(owny, owny, send_sem.at[17 + i], agy_sem.at[me], p)
        copy.start()
        sent.append(copy)

    peak[...] = jnp.full(peak.shape, -jnp.inf, jnp.float32)
    total[...] = jnp.zeros(total.shape, jnp.float32)
    lanes = peak.shape[1]

    def head_stats(rows, buf):
        old = peak[rows, :]
        new = old
        for c in range(0, wide, lanes):
            new = jnp.maximum(new, buf[:, c:c + lanes])
        acc = total[rows, :] * jnp.exp(old - new)
        for c in range(0, wide, lanes):
            acc = acc + jnp.exp(buf[:, c:c + lanes] - new)
        peak[rows, :] = new
        total[rows, :] = acc

    def head_loop(rows, size, lo, hi, before, after):
        def stage(g, i):
            return zst.at[lax.rem(g, 2), i, pl.ds(0, size), :]

        def copy_z(g, i):
            return pltpu.make_async_copy(stage(g, i), z_hbm.at[rows, cols(GROUP * g + i)], zout_sem.at[lax.rem(g, 2), i])

        def body(g, carry):
            for i in range(GROUP):
                before(GROUP * g + i)

            @pl.when(g >= lo + 2)
            def _():
                for i in range(GROUP):
                    copy_z(g - 2, i).wait()

            for i in range(GROUP):
                stage(g, i)[...] = jnp.dot(hf[rows, :], slots[lax.rem(GROUP * g + i + first_out, count)], preferred_element_type=jnp.float32)
                head_stats(rows, stage(g, i))
            for i in range(GROUP):
                copy_z(g, i).start()
            after(g)
            return carry

        lax.fori_loop(lo, hi, body, 0)
        for g in range(max(lo, hi - 2), hi):
            for i in range(GROUP):
                copy_z(g, i).wait()

    def nothing(j):
        pass

    def next_out(g):
        for i in range(GROUP):
            @pl.when(GROUP * g + i + count < n_out)
            def _():
                load_out(GROUP * g + i + count).start()

    def ready(j):
        load_out(j).wait()

    for s in range(2):
        arrived(hf.at[half_of(partner, s), :], agf_sem, 2 * partner + s)
    relays = [push(hf.at[half_of(cross, s), :], hf.at[half_of(cross, s), :], send_sem.at[19 + s], agf_sem.at[2 * cross + s], partner) for s in range(2)]

    def pass_on(g):
        for s in range(2):
            @pl.when(g == s)
            def _():
                arrived(hf.at[half_of(cross, s), :], agf_sem, 2 * cross + s)
                relays[s].start()

    head_loop(local, half, 0, EARLY, ready, pass_on)
    sent += relays
    for s in range(2):
        arrived(hf.at[half_of(diag, s), :], agf_sem, 2 * diag + s)
    head_loop(remote, half, 0, EARLY, nothing, next_out)
    arrived(y_ref.at[rows_of(cross), :], agy_sem, cross)
    relayy = push(y_ref.at[rows_of(cross), :], y_ref.at[rows_of(cross), :], send_sem.at[21], agy_sem.at[cross], partner)
    relayy.start()
    head_loop(pl.ds(0, batch), batch, EARLY, n_out // GROUP, ready, next_out)

    for p in (partner, diag):
        arrived(y_ref.at[rows_of(p), :], agy_sem, p)
    y_copy = pltpu.make_async_copy(y_ref, y_hbm, load_sem.at[0])
    y_copy.start()
    top = jnp.max(peak[...], axis=1, keepdims=True)
    bottom = jnp.sum(total[...] * jnp.exp(peak[...] - top), axis=1, keepdims=True)
    stats[me, 0] = jnp.broadcast_to(top, peak.shape).T[0:8]
    stats[me, 1] = jnp.broadcast_to(bottom, peak.shape).T[0:8]
    st = [push(stats.at[me], stats.at[me], send_sem.at[22 + i], st_sem.at[me], p) for i, p in enumerate((cross, diag, partner))]
    for copy in st:
        copy.start()
    for p in (partner, cross, diag):
        arrived(stats.at[p], st_sem, p)
    tops = [stats[i, 0] for i in range(4)]
    whole_top = jnp.maximum(jnp.maximum(tops[0], tops[1]), jnp.maximum(tops[2], tops[3]))
    whole = sum(stats[i, 1] * jnp.exp(tops[i] - whole_top) for i in range(4))
    lse = whole_top + jnp.log(whole)
    lse_ref[...] = jnp.broadcast_to(lse[0:1], (lanes, batch)).T

    y_copy.wait()
    for copy in sent + [relayy] + st:
        copy.wait_send()
    for i, p in enumerate((cross, diag)):
        for s in range(2):
            whole_half = part2.at[half_of(p, s), :]
            push(whole_half, recv2.at[me, pl.ds(sub * s, sub), :], send_sem.at[5 + 2 * i + s], rs2_sem.at[2 * me + s], p).wait_send()


def subtract_kernel(lse_ref, hidden_hbm, logits_hbm, y_hbm, logp_hbm, y_buf, buf, y_sem, in_sem, out_sem):
    blocks, rows, _ = buf.shape
    ins = [pltpu.make_async_copy(logits_hbm.at[pl.ds(rows * i, rows), :], buf.at[i], in_sem.at[i]) for i in range(blocks)]
    outs = [pltpu.make_async_copy(buf.at[i], logp_hbm.at[pl.ds(rows * i, rows), :], out_sem.at[i]) for i in range(blocks)]
    y_in = pltpu.make_async_copy(hidden_hbm, y_buf, y_sem.at[0])
    y_out = pltpu.make_async_copy(y_buf, y_hbm, y_sem.at[1])
    for copy in ins:
        copy.start()
    y_in.start()
    for i in range(blocks):
        ins[i].wait()
        buf[i] = buf[i] - lse_ref[rows * i:rows * (i + 1), 0:1]
        outs[i].start()
    y_in.wait()
    y_out.start()
    for copy in outs + [y_out]:
        copy.wait()


def finish_layer(partials, new_hidden, ln2_gain, ln2_bias, lnf_gain, lnf_bias, w_up, w_down, w_out):
    batch, width = new_hidden.shape
    own_rows = batch // 4
    vocab = w_out.shape[1]
    vmem = pl.BlockSpec(memory_space=pltpu.VMEM)
    hbm = pl.BlockSpec(memory_space=pl.ANY)
    dma = pltpu.SemaphoreType.DMA
    bf16, f32 = jnp.bfloat16, jnp.float32
    hidden, logits, lse = pl.pallas_call(
        layer_kernel,
        out_shape=(jax.ShapeDtypeStruct((batch, width), bf16), jax.ShapeDtypeStruct((batch, vocab), f32), jax.ShapeDtypeStruct((batch, 128), f32)),
        in_specs=[vmem] * 8 + [hbm] * 3,
        out_specs=(hbm, hbm, vmem),
        scratch_shapes=[
            pltpu.VMEM((batch, width), bf16),
            pltpu.VMEM((SLOTS, width, WIDE), bf16),
            pltpu.VMEM((own_rows, width), bf16),
            pltpu.VMEM((4, own_rows, width), bf16),
            pltpu.VMEM((batch, width), bf16),
            pltpu.VMEM((2 * own_rows, w_up.shape[1]), bf16),
            pltpu.VMEM((own_rows, w_up.shape[1]), bf16),
            pltpu.VMEM((batch, width), bf16),
            pltpu.VMEM((batch, width), bf16),
            pltpu.VMEM((own_rows, width), bf16),
            pltpu.VMEM((2, GROUP, batch, WIDE), f32),
            pltpu.VMEM((batch, 128), f32),
            pltpu.VMEM((batch, 128), f32),
            pltpu.VMEM((4, 2, 8, batch), f32),
            dma((1,)), dma((SLOTS,)), dma((2, GROUP)), dma((25,)), dma((1,)), dma((8,)), dma((8,)), dma((8,)), dma((4,)), dma((4,)),
        ],
        compiler_params=pltpu.CompilerParams(vmem_limit_bytes=VMEM_LIMIT, collective_id=0, has_side_effects=True),
        cost_estimate=pl.CostEstimate(flops=2 * batch * (w_up.size + w_down.size + w_out.size), bytes_accessed=2 * (w_up.size + w_down.size + w_out.size), transcendentals=batch * vocab),
        name="layer",
    )(*partials, ln2_gain, ln2_bias, lnf_gain, lnf_bias, w_up, w_down, w_out)
    blocks = 16
    return pl.pallas_call(
        subtract_kernel,
        out_shape=(jax.ShapeDtypeStruct((batch, width), bf16), jax.ShapeDtypeStruct((batch, vocab), f32)),
        in_specs=[vmem, hbm, hbm],
        out_specs=(hbm, hbm),
        scratch_shapes=[pltpu.VMEM((batch, width), bf16), pltpu.VMEM((blocks, batch // blocks, vocab), f32), dma((2,)), dma((blocks,)), dma((blocks,))],
        compiler_params=pltpu.CompilerParams(vmem_limit_bytes=VMEM_LIMIT),
        cost_estimate=pl.CostEstimate(flops=batch * vocab, bytes_accessed=8 * batch * vocab, transcendentals=0),
        name="subtract",
    )(lse, hidden, logits)


def solution(mesh):
    row_spec = P('bs', None)
    cache_spec = P('bs', None, 'tp', None)
    col_split = P(None, 'tp')
    row_split = P('tp', None)
    in_specs = (row_spec, cache_spec, cache_spec, P('bs'), P(), P(), col_split, col_split, col_split, row_split, P(), P(), col_split, row_split, P(), P(), col_split)
    out_specs = (P('bs', 'tp'), cache_spec, cache_spec, row_spec)

    def local_step(new_hidden, cache_k, cache_v, lengths, ln1_gain, ln1_bias, w_q, w_k, w_v, w_o, ln2_gain, ln2_bias, w_up, w_down, lnf_gain, lnf_bias, w_out):
        partials, new_cache_k, new_cache_v = attend(new_hidden, cache_k, cache_v, lengths, ln1_gain, ln1_bias, w_q, w_k, w_v, w_o)
        out_hidden, log_probs = finish_layer(partials, new_hidden, ln2_gain, ln2_bias, lnf_gain, lnf_bias, w_up, w_down, w_out)
        return log_probs, new_cache_k, new_cache_v, out_hidden

    return jax.shard_map(local_step, mesh=mesh, in_specs=in_specs, out_specs=out_specs, check_vma=False)
```

```python
import math
import jax
import jax.numpy as jnp
from jax import lax
from jax.experimental import pallas as pl
from jax.experimental.pallas import tpu as pltpu
from jax.sharding import PartitionSpec as P

EPSILON = 1e-5
ROPE_BASE = 10000.0
AHEAD_FAR = 5
AHEAD_NEAR = 5
WIDE = 512
SLOTS = 18
GROUP = 5
WINDOW = 4
EARLY = 3
VMEM_LIMIT = 66 * 1000 * 1000


def norm_block(values, gain, bias):
    mean = jnp.mean(values, axis=-1, keepdims=True)
    centered = values - mean
    variance = jnp.mean(jnp.square(centered), axis=-1, keepdims=True)
    return centered * lax.rsqrt(variance + EPSILON) * (1.0 + gain) + bias


def attend_lanes(start, ahead, lengths, project, part, kc_hbm, vc_hbm, ko_hbm, vo_hbm, kbuf, vbuf, attn_ref, s_ref, ki_sem, vi_sem, ko_sem, vo_sem):
    heads, cache_len, head_dim, batch = kbuf.shape
    lanes = pl.ds(pl.multiple_of(start, batch), batch)

    def k_in(h):
        return pltpu.make_async_copy(kc_hbm.at[:, h, :, lanes], kbuf.at[h], ki_sem.at[h])

    def v_in(h):
        return pltpu.make_async_copy(vc_hbm.at[:, h, :, lanes], vbuf.at[h], vi_sem.at[h])

    def k_out(h):
        return pltpu.make_async_copy(kbuf.at[h], ko_hbm.at[:, h, :, lanes], ko_sem.at[h])

    def v_out(h):
        return pltpu.make_async_copy(vbuf.at[h], vo_hbm.at[:, h, :, lanes], vo_sem.at[h])

    for h in range(ahead):
        k_in(h).start()
        v_in(h).start()
    qkv = project()
    scale = head_dim ** -0.5

    def one_head(h, carry):
        @pl.when(h + ahead < heads)
        def _():
            k_in(h + ahead).start()
            v_in(h + ahead).start()

        here = pl.ds(pl.multiple_of(h * head_dim, head_dim), head_dim)
        query = qkv[0, here, :].astype(jnp.bfloat16).astype(jnp.float32)
        key_new = qkv[1, here, :].astype(jnp.bfloat16)
        val_new = qkv[2, here, :].astype(jnp.bfloat16)
        k_in(h).wait()

        def score_row(l, c):
            old = kbuf[h, l]
            row = jnp.where(jnp.broadcast_to(lengths == l, old.shape), key_new, old)
            kbuf[h, l] = row
            s_ref[pl.ds(l, 1), :] = jnp.sum(row.astype(jnp.float32) * query, axis=0, keepdims=True)
            return c

        lax.fori_loop(0, cache_len, score_row, 0, unroll=8)
        k_out(h).start()
        scores = s_ref[...] * scale
        valid = lax.broadcasted_iota(jnp.int32, scores.shape, 0) <= lengths
        scores = jnp.where(valid, scores, -1e30)
        weights = jnp.exp(scores - jnp.max(scores, axis=0, keepdims=True))
        s_ref[...] = (weights / jnp.sum(weights, axis=0, keepdims=True)).astype(jnp.bfloat16).astype(jnp.float32)
        v_in(h).wait()

        def mix_row(l, acc):
            old = vbuf[h, l]
            row = jnp.where(jnp.broadcast_to(lengths == l, old.shape), val_new, old)
            vbuf[h, l] = row
            return acc + s_ref[pl.ds(l, 1), :] * row.astype(jnp.float32)

        attn_ref[here, :] = lax.fori_loop(0, cache_len, mix_row, jnp.zeros((head_dim, batch), jnp.float32), unroll=8)
        v_out(h).start()
        return carry

    lax.fori_loop(0, heads, one_head, 0)
    part(attn_ref[...].T.astype(jnp.bfloat16))
    for h in range(heads):
        k_out(h).wait()
        v_out(h).wait()


def far_kernel(x_ref, len_ref, gain_ref, bias_ref, wq_hbm, wk_hbm, wv_hbm, wo_hbm, kc_hbm, vc_hbm, cross_ref, diag_ref, near_ref, own_ref, ko_hbm, vo_hbm, kbuf, vbuf, wbuf, wobuf, h_ref, qkv_ref, tmp_ref, attn_ref, s_ref, far_ref, w_sem, ki_sem, vi_sem, ko_sem, vo_sem):
    heads, cache_len, head_dim, half = kbuf.shape
    batch = x_ref.shape[0]
    half_rot = head_dim // 4
    me = lax.axis_index("tp")
    chip = me // 2
    core = lax.rem(me, 2)
    copies = [pltpu.make_async_copy(src, wbuf.at[i], w_sem.at[i]) for i, src in enumerate((wq_hbm, wk_hbm, wv_hbm))]
    wo_copy = pltpu.make_async_copy(wo_hbm, wobuf, w_sem.at[3])
    for copy in copies:
        copy.start()
    own_rows = half // 2
    own_ref[...] = x_ref[pl.ds(pl.multiple_of(own_rows * me, own_rows), own_rows), :]
    rows = 32
    gain, bias = gain_ref[...][None, :], bias_ref[...][None, :]

    def project():
        def norm_rows(i, carry):
            here = pl.ds(pl.multiple_of(i * rows, rows), rows)
            h_ref[here, :] = norm_block(x_ref[here, :].astype(jnp.float32), gain, bias).astype(jnp.bfloat16)
            return carry

        lax.fori_loop(0, batch // rows, norm_rows, 0)
        index = lax.broadcasted_iota(jnp.int32, (2 * half_rot, batch), 0)
        upper = index < half_rot
        pair = jnp.where(upper, index, index - half_rot).astype(jnp.float32)
        angles = jnp.exp(pair * (-math.log(ROPE_BASE) / half_rot)) * len_ref[...].astype(jnp.float32)
        cosine = jnp.cos(angles)
        sine = jnp.where(upper, -jnp.sin(angles), jnp.sin(angles))
        for i in range(3):
            copies[i].wait()
            tmp_ref[...] = jnp.dot(h_ref[...], wbuf[i], preferred_element_type=jnp.float32).T
            for h in range(heads):
                base = h * head_dim
                if i == 2:
                    blocks = [(base, head_dim, tmp_ref[pl.ds(base, head_dim), :])]
                else:
                    first = tmp_ref[pl.ds(base, half_rot), :]
                    second = tmp_ref[pl.ds(base + half_rot, half_rot), :]
                    both = tmp_ref[pl.ds(base, 2 * half_rot), :]
                    swapped = jnp.concatenate([second, first], axis=0)
                    rest = head_dim - 2 * half_rot
                    blocks = [(base, 2 * half_rot, both * cosine + swapped * sine), (base + 2 * half_rot, rest, tmp_ref[pl.ds(base + 2 * half_rot, rest), :])]
                for at, size, value in blocks:
                    qkv_ref[0, i, pl.ds(at, size), :] = value[:, :half]
                    qkv_ref[1, i, pl.ds(at, size), :] = value[:, half:]
        wo_copy.start()
        near_ref[...] = qkv_ref[chip]
        return qkv_ref.at[1 - chip]

    def part(attended):
        wo_copy.wait()
        wide = 512
        for n in range(0, far_ref.shape[1], wide):
            far_ref[:, n:n + wide] = jnp.dot(attended, wobuf[:, n:n + wide], preferred_element_type=jnp.float32).astype(jnp.bfloat16)
        own = half // 2
        cross_ref[...] = far_ref[pl.ds(pl.multiple_of(own * core, own), own), :]
        diag_ref[...] = far_ref[pl.ds(pl.multiple_of(own * (1 - core), own), own), :]

    start = half * (1 - chip)
    lengths = len_ref[:, pl.ds(pl.multiple_of(start, half), half)]
    attend_lanes(start, AHEAD_FAR, lengths, project, part, kc_hbm, vc_hbm, ko_hbm, vo_hbm, kbuf, vbuf, attn_ref, s_ref, ki_sem, vi_sem, ko_sem, vo_sem)


def near_kernel(len_ref, qkv_ref, wo_hbm, kc_hbm, vc_hbm, ko_in, vo_in, part_ref, ko_hbm, vo_hbm, kbuf, vbuf, wobuf, attn_ref, s_ref, w_sem, ki_sem, vi_sem, ko_sem, vo_sem):
    half = kbuf.shape[3]
    chip = lax.axis_index("tp") // 2
    start = half * chip
    lengths = len_ref[:, pl.ds(pl.multiple_of(start, half), half)]
    wo_copy = pltpu.make_async_copy(wo_hbm, wobuf, w_sem.at[0])

    def project():
        wo_copy.start()
        return qkv_ref

    def part(attended):
        wo_copy.wait()
        wide = 512
        for n in range(0, part_ref.shape[1], wide):
            part_ref[:, n:n + wide] = jnp.dot(attended, wobuf[:, n:n + wide], preferred_element_type=jnp.float32).astype(jnp.bfloat16)

    attend_lanes(start, AHEAD_NEAR, lengths, project, part, kc_hbm, vc_hbm, ko_hbm, vo_hbm, kbuf, vbuf, attn_ref, s_ref, ki_sem, vi_sem, ko_sem, vo_sem)


def attend(new_hidden, cache_k, cache_v, lengths, ln1_gain, ln1_bias, w_q, w_k, w_v, w_o):
    batch, cache_len, heads, head_dim = cache_k.shape
    width = new_hidden.shape[1]
    flat = heads * head_dim
    half = batch // 2
    k_view = jnp.transpose(cache_k, (1, 2, 3, 0))
    v_view = jnp.transpose(cache_v, (1, 2, 3, 0))
    vmem = pl.BlockSpec(memory_space=pltpu.VMEM)
    hbm = pl.BlockSpec(memory_space=pl.ANY)
    dma = pltpu.SemaphoreType.DMA
    bf16, f32 = jnp.bfloat16, jnp.float32
    shape = jax.ShapeDtypeStruct
    lens = lengths[None, :]
    slabs = [pltpu.VMEM((heads, cache_len, head_dim, half), bf16)] * 2
    sems = [dma((heads,))] * 4
    to_cross, to_diag, near, own, k_half, v_half = pl.pallas_call(
        far_kernel,
        out_shape=(shape((half // 2, width), bf16), shape((half // 2, width), bf16), shape((3, flat, half), f32), shape((half // 2, width), bf16), shape(k_view.shape, bf16), shape(v_view.shape, bf16)),
        in_specs=[vmem] * 4 + [hbm] * 6,
        out_specs=(vmem, vmem, vmem, vmem, hbm, hbm),
        scratch_shapes=slabs + [
            pltpu.VMEM((3, width, flat), bf16),
            pltpu.VMEM((flat, width), bf16),
            pltpu.VMEM((batch, width), bf16),
            pltpu.VMEM((2, 3, flat, half), f32),
            pltpu.VMEM((flat, batch), f32),
            pltpu.VMEM((flat, half), f32),
            pltpu.VMEM((cache_len, half), f32),
            pltpu.VMEM((half, width), bf16),
            dma((4,)),
        ] + sems,
        compiler_params=pltpu.CompilerParams(vmem_limit_bytes=VMEM_LIMIT),
        cost_estimate=pl.CostEstimate(flops=8 * batch * width * flat, bytes_accessed=4 * cache_k.size + 8 * width * flat, transcendentals=0),
        name="far",
    )(new_hidden, lens, ln1_gain, ln1_bias, w_q, w_k, w_v, w_o, k_view, v_view)
    from_cross = lax.ppermute(to_cross, "tp", [(i, (i + 2) % 4) for i in range(4)])
    from_diag = lax.ppermute(to_diag, "tp", [(i, 3 - i) for i in range(4)])
    partial, k_new, v_new = pl.pallas_call(
        near_kernel,
        out_shape=(shape((half, width), bf16), shape(k_view.shape, bf16), shape(v_view.shape, bf16)),
        in_specs=[vmem] * 2 + [hbm] * 5,
        out_specs=(vmem, hbm, hbm),
        input_output_aliases={5: 1, 6: 2},
        scratch_shapes=slabs + [
            pltpu.VMEM((flat, width), bf16),
            pltpu.VMEM((flat, half), f32),
            pltpu.VMEM((cache_len, half), f32),
            dma((1,)),
        ] + sems,
        compiler_params=pltpu.CompilerParams(vmem_limit_bytes=VMEM_LIMIT),
        cost_estimate=pl.CostEstimate(flops=40 * batch * width * flat, bytes_accessed=4 * cache_k.size, transcendentals=0),
        name="near",
    )(lens, near, w_o, k_view, v_view, k_half, v_half)
    return (partial, from_cross, from_diag, own), jnp.transpose(k_new, (3, 0, 1, 2)), jnp.transpose(v_new, (3, 0, 1, 2))


def layer_kernel(near_ref, cross_ref, diag_ref, xrow, gain2_ref, bias2_ref, gainf_ref, biasf_ref, up_hbm, down_hbm, out_hbm, y_hbm, z_hbm, lse_ref, y_ref, slots, recv, recv2, h2, act, act_far, part2, hf, x1, zst, peak, total, stats, load_sem, slot_sem, zout_sem, send_sem, rs_sem, ag_sem, rs2_sem, agf_sem, agy_sem, st_sem):
    batch, width = y_ref.shape
    own_rows = x1.shape[0]
    half = 2 * own_rows
    sub = own_rows // 2
    count, _, wide = slots.shape
    n_up = up_hbm.shape[1] // wide
    n_down = down_hbm.shape[1] // wide
    n_out = out_hbm.shape[1] // wide
    first_out = n_up + n_down
    me = lax.axis_index("tp")
    chip = me // 2
    core = lax.rem(me, 2)
    partner = 2 * chip + 1 - core
    cross = 2 * (1 - chip) + core
    diag = 2 * (1 - chip) + 1 - core
    local = pl.ds(pl.multiple_of(half * chip, half), half)
    remote = pl.ds(pl.multiple_of(half * (1 - chip), half), half)

    def rows_of(owner):
        return pl.ds(pl.multiple_of(own_rows * owner, own_rows), own_rows)

    def cols(n):
        return pl.ds(pl.multiple_of(n * wide, wide), wide)

    def push(src, dst, sem, recv_sem, to):
        return pltpu.make_async_remote_copy(src_ref=src, dst_ref=dst, send_sem=sem, recv_sem=recv_sem, device_id={"tp": to}, device_id_type=pl.DeviceIdType.MESH)

    def load_up(n):
        return pltpu.make_async_copy(up_hbm.at[:, cols(n)], slots.at[n], slot_sem.at[n])

    def load_down(n):
        return pltpu.make_async_copy(down_hbm.at[:, cols(n)], slots.at[n_up + n], slot_sem.at[n_up + n])

    def load_out(j):
        slot = lax.rem(j + first_out, count)
        return pltpu.make_async_copy(out_hbm.at[:, cols(j)], slots.at[slot], slot_sem.at[slot])

    def half_of(owner, s):
        return pl.ds(pl.multiple_of(own_rows * owner + sub * s, sub), sub)

    barrier = pltpu.get_barrier_semaphore()
    for other in (partner, cross, diag):
        pl.semaphore_signal(barrier, inc=1, device_id={"tp": other}, device_id_type=pl.DeviceIdType.MESH)
    for n in range(n_up):
        load_up(n).start()
    for n in range(n_down):
        load_down(n).start()
    pl.semaphore_wait(barrier, 3)

    rs = push(near_ref.at[rows_of(1 - core), :], recv, send_sem.at[0], rs_sem.at[0], partner)
    rs.start()

    def arrived(ref, sem, index):
        pltpu.make_async_copy(ref, ref, sem.at[index]).wait()

    def share(ref, sem, s, first_send):
        rows = ref.at[half_of(me, s), :]
        to_cross = push(rows, rows, send_sem.at[first_send], sem.at[2 * me + s], cross)
        to_partner = push(rows, rows, send_sem.at[first_send + 1], sem.at[2 * me + s], partner)
        to_cross.start()
        to_partner.start()
        return [to_cross, to_partner]

    def relay(ref, sem, s, first_send):
        rows = ref.at[half_of(cross, s), :]
        arrived(rows, sem, 2 * cross + s)
        copy = push(rows, rows, send_sem.at[first_send], sem.at[2 * cross + s], partner)
        copy.start()
        return [copy]

    sent = [rs]
    gain2, bias2 = gain2_ref[...][None, :], bias2_ref[...][None, :]
    arrived(recv, rs_sem, 0)
    for s in range(2):
        here = pl.ds(sub * s, sub)
        summed = near_ref[half_of(core, s), :].astype(jnp.float32)
        for other in (recv, cross_ref, diag_ref):
            summed = summed + other[here, :].astype(jnp.float32)
        mid = (xrow[here, :].astype(jnp.float32) + summed).astype(jnp.bfloat16)
        x1[here, :] = mid
        h2[half_of(me, s), :] = norm_block(mid.astype(jnp.float32), gain2, bias2).astype(jnp.bfloat16)
        sent += share(h2, ag_sem, s, 1 + 2 * s)

    def far_rows(ref, s, columns):
        return jnp.concatenate([ref[half_of(2 * (1 - chip), s), columns], ref[half_of(2 * (1 - chip) + 1, s), columns]], axis=0)

    def squared(up):
        return jnp.square(jnp.maximum(up, 0.0)).astype(jnp.bfloat16)

    def up_near():
        for n in range(n_up):
            act[:, wide * n:wide * (n + 1)] = squared(jnp.dot(h2[local, :], slots[n], preferred_element_type=jnp.float32))

    def up_far(s):
        for n in range(n_up):
            act_far[:, wide * n:wide * (n + 1)] = squared(jnp.dot(far_rows(h2, s, slice(None)), slots[n], preferred_element_type=jnp.float32))

    def down_near():
        for n in range(n_down):
            part2[local, wide * n:wide * (n + 1)] = jnp.dot(act[...], slots[n_up + n], preferred_element_type=jnp.float32).astype(jnp.bfloat16)

    def send_far(p, i, s, n):
        return push(part2.at[half_of(p, s), cols(n)], recv2.at[me, pl.ds(sub * s, sub), cols(n)], send_sem.at[5 + 2 * i + s], rs2_sem.at[2 * me + s], p)

    def down_far(s):
        for lo, hi in ((0, 1), (1, 3), (3, n_down)):
            for n in range(lo, hi):
                down = jnp.dot(act_far[...], slots[n_up + n], preferred_element_type=jnp.float32).astype(jnp.bfloat16)
                part2[half_of(2 * (1 - chip), s), wide * n:wide * (n + 1)] = down[:sub]
                part2[half_of(2 * (1 - chip) + 1, s), wide * n:wide * (n + 1)] = down[sub:]
            for n in range(lo, hi):
                for i, p in enumerate((cross, diag)):
                    send_far(p, i, s, n).start()

    for s in range(2):
        arrived(h2.at[half_of(partner, s), :], ag_sem, 2 * partner + s)
    for n in range(n_up):
        load_up(n).wait()
    for j in range(count - first_out):
        load_out(j).start()
    up_near()
    sent += relay(h2, ag_sem, 0, 9)
    arrived(h2.at[half_of(diag, 0), :], ag_sem, 2 * diag)
    up_far(0)
    sent += relay(h2, ag_sem, 1, 10)
    for n in range(n_down):
        load_down(n).wait()
    down_far(0)
    arrived(h2.at[half_of(diag, 1), :], ag_sem, 2 * diag + 1)
    up_far(1)
    for j in range(count - first_out, count - n_down):
        load_out(j).start()
    down_far(1)
    down_near()
    for j in range(count - n_down, count):
        load_out(j).start()
    for s in range(2):
        copy = push(part2.at[half_of(partner, s), :], recv2.at[me, pl.ds(sub * s, sub), :], send_sem.at[11 + s], rs2_sem.at[2 * me + s], partner)
        copy.start()
        sent.append(copy)

    gainf, biasf = gainf_ref[...][None, :], biasf_ref[...][None, :]
    for s in range(2):
        here = pl.ds(sub * s, sub)
        for p in (partner, cross, diag):
            arrived(recv2.at[p, here, :], rs2_sem, 2 * p + s)
        summed = part2[half_of(me, s), :].astype(jnp.float32)
        for p in (partner, cross, diag):
            summed = summed + recv2[p, here, :].astype(jnp.float32)
        out = (x1[here, :].astype(jnp.float32) + summed).astype(jnp.bfloat16)
        y_ref[half_of(me, s), :] = out
        hf[half_of(me, s), :] = norm_block(out.astype(jnp.float32), gainf, biasf).astype(jnp.bfloat16)
        sent += share(hf, agf_sem, s, 13 + 2 * s)
    owny = y_ref.at[rows_of(me), :]
    for i, p in enumerate((cross, partner)):
        copy = push(owny, owny, send_sem.at[17 + i], agy_sem.at[me], p)
        copy.start()
        sent.append(copy)

    peak[...] = jnp.full(peak.shape, -jnp.inf, jnp.float32)
    total[...] = jnp.zeros(total.shape, jnp.float32)
    lanes = peak.shape[1]

    def head_stats(rows, buf):
        old = peak[rows, :]
        new = old
        for c in range(0, wide, lanes):
            new = jnp.maximum(new, buf[:, c:c + lanes])
        acc = total[rows, :] * jnp.exp(old - new)
        for c in range(0, wide, lanes):
            acc = acc + jnp.exp(buf[:, c:c + lanes] - new)
        peak[rows, :] = new
        total[rows, :] = acc

    everyone = pl.ds(0, batch)
    turns = [(local, half, g) for g in range(EARLY)] + [(remote, half, g) for g in range(EARLY)] + [(everyone, batch, g) for g in range(EARLY, n_out // GROUP)]

    def copy_z(rows, size, g, parity, i):
        return pltpu.make_async_copy(zst.at[parity, i, pl.ds(0, size), :], z_hbm.at[rows, cols(GROUP * g + i)], zout_sem.at[parity, i])

    def finish_turn(turn):
        rows, size, g = turns[turn]
        for i in range(GROUP):
            copy_z(rows, size, g, turn % 2, i).wait()

    def head_loop(first, last, before, after):
        rows, size, lo = turns[first]
        hi = turns[last][2] + 1

        def body(g, carry):
            parity = lax.rem(g - lo + first, 2)
            for i in range(GROUP):
                before(GROUP * g + i)
            for ago in range(2):
                if first + ago >= 2:
                    @pl.when(g == lo + ago)
                    def _():
                        finish_turn(first + ago - 2)

            @pl.when(g >= lo + 2)
            def _():
                for i in range(GROUP):
                    copy_z(rows, size, g - 2, parity, i).wait()

            for i in range(GROUP):
                stage = zst.at[parity, i, pl.ds(0, size), :]
                stage[...] = jnp.dot(hf[rows, :], slots[lax.rem(GROUP * g + i + first_out, count)], preferred_element_type=jnp.float32)
                head_stats(rows, stage)
            for i in range(GROUP):
                copy_z(rows, size, g, parity, i).start()
            after(g)
            return carry

        lax.fori_loop(lo, hi, body, 0)

    def nothing(j):
        pass

    def next_out(g):
        for i in range(GROUP):
            @pl.when(GROUP * g + i + count < n_out)
            def _():
                load_out(GROUP * g + i + count).start()

    def ready(j):
        load_out(j).wait()

    for s in range(2):
        arrived(hf.at[half_of(partner, s), :], agf_sem, 2 * partner + s)
    relays = [push(hf.at[half_of(cross, s), :], hf.at[half_of(cross, s), :], send_sem.at[19 + s], agf_sem.at[2 * cross + s], partner) for s in range(2)]

    def pass_on(g):
        for s in range(2):
            @pl.when(g == s)
            def _():
                arrived(hf.at[half_of(cross, s), :], agf_sem, 2 * cross + s)
                relays[s].start()

    head_loop(0, EARLY - 1, ready, pass_on)
    sent += relays
    for s in range(2):
        arrived(hf.at[half_of(diag, s), :], agf_sem, 2 * diag + s)
    head_loop(EARLY, 2 * EARLY - 1, nothing, next_out)
    arrived(y_ref.at[rows_of(cross), :], agy_sem, cross)
    relayy = push(y_ref.at[rows_of(cross), :], y_ref.at[rows_of(cross), :], send_sem.at[21], agy_sem.at[cross], partner)
    relayy.start()
    head_loop(2 * EARLY, len(turns) - 1, ready, next_out)

    for p in (partner, diag):
        arrived(y_ref.at[rows_of(p), :], agy_sem, p)
    y_copy = pltpu.make_async_copy(y_ref, y_hbm, load_sem.at[0])
    y_copy.start()
    top = jnp.max(peak[...], axis=1, keepdims=True)
    bottom = jnp.sum(total[...] * jnp.exp(peak[...] - top), axis=1, keepdims=True)
    stats[me, 0] = jnp.broadcast_to(top, peak.shape).T[0:8]
    stats[me, 1] = jnp.broadcast_to(bottom, peak.shape).T[0:8]
    st = [push(stats.at[me], stats.at[me], send_sem.at[22 + i], st_sem.at[me], p) for i, p in enumerate((cross, diag, partner))]
    for copy in st:
        copy.start()
    for p in (partner, cross, diag):
        arrived(stats.at[p], st_sem, p)
    tops = [stats[i, 0] for i in range(4)]
    whole_top = jnp.maximum(jnp.maximum(tops[0], tops[1]), jnp.maximum(tops[2], tops[3]))
    whole = sum(stats[i, 1] * jnp.exp(tops[i] - whole_top) for i in range(4))
    lse = whole_top + jnp.log(whole)
    lse_ref[...] = jnp.broadcast_to(lse[0:1], (lanes, batch)).T

    for turn in (len(turns) - 2, len(turns) - 1):
        finish_turn(turn)
    y_copy.wait()
    for copy in sent + [relayy] + st:
        copy.wait_send()
    for i, p in enumerate((cross, diag)):
        for s in range(2):
            whole_half = part2.at[half_of(p, s), :]
            push(whole_half, recv2.at[me, pl.ds(sub * s, sub), :], send_sem.at[5 + 2 * i + s], rs2_sem.at[2 * me + s], p).wait_send()


def subtract_kernel(lse_ref, hidden_hbm, logits_hbm, y_hbm, logp_hbm, y_buf, buf, y_sem, in_sem, out_sem):
    blocks, rows, _ = buf.shape
    ins = [pltpu.make_async_copy(logits_hbm.at[pl.ds(rows * i, rows), :], buf.at[i], in_sem.at[i]) for i in range(blocks)]
    outs = [pltpu.make_async_copy(buf.at[i], logp_hbm.at[pl.ds(rows * i, rows), :], out_sem.at[i]) for i in range(blocks)]
    y_in = pltpu.make_async_copy(hidden_hbm, y_buf, y_sem.at[0])
    y_out = pltpu.make_async_copy(y_buf, y_hbm, y_sem.at[1])
    for copy in ins[:WINDOW]:
        copy.start()
    y_in.start()
    for i in range(blocks):
        if i + WINDOW < blocks:
            ins[i + WINDOW].start()
        ins[i].wait()
        buf[i] = buf[i] - lse_ref[rows * i:rows * (i + 1), 0:1]
        outs[i].start()
    y_in.wait()
    y_out.start()
    for copy in outs + [y_out]:
        copy.wait()


def finish_layer(partials, new_hidden, ln2_gain, ln2_bias, lnf_gain, lnf_bias, w_up, w_down, w_out):
    batch, width = new_hidden.shape
    own_rows = batch // 4
    vocab = w_out.shape[1]
    vmem = pl.BlockSpec(memory_space=pltpu.VMEM)
    hbm = pl.BlockSpec(memory_space=pl.ANY)
    dma = pltpu.SemaphoreType.DMA
    bf16, f32 = jnp.bfloat16, jnp.float32
    hidden, logits, lse = pl.pallas_call(
        layer_kernel,
        out_shape=(jax.ShapeDtypeStruct((batch, width), bf16), jax.ShapeDtypeStruct((batch, vocab), f32), jax.ShapeDtypeStruct((batch, 128), f32)),
        in_specs=[vmem] * 8 + [hbm] * 3,
        out_specs=(hbm, hbm, vmem),
        scratch_shapes=[
            pltpu.VMEM((batch, width), bf16),
            pltpu.VMEM((SLOTS, width, WIDE), bf16),
            pltpu.VMEM((own_rows, width), bf16),
            pltpu.VMEM((4, own_rows, width), bf16),
            pltpu.VMEM((batch, width), bf16),
            pltpu.VMEM((2 * own_rows, w_up.shape[1]), bf16),
            pltpu.VMEM((own_rows, w_up.shape[1]), bf16),
            pltpu.VMEM((batch, width), bf16),
            pltpu.VMEM((batch, width), bf16),
            pltpu.VMEM((own_rows, width), bf16),
            pltpu.VMEM((2, GROUP, batch, WIDE), f32),
            pltpu.VMEM((batch, 128), f32),
            pltpu.VMEM((batch, 128), f32),
            pltpu.VMEM((4, 2, 8, batch), f32),
            dma((1,)), dma((SLOTS,)), dma((2, GROUP)), dma((25,)), dma((1,)), dma((8,)), dma((8,)), dma((8,)), dma((4,)), dma((4,)),
        ],
        compiler_params=pltpu.CompilerParams(vmem_limit_bytes=VMEM_LIMIT, collective_id=0, has_side_effects=True),
        cost_estimate=pl.CostEstimate(flops=2 * batch * (w_up.size + w_down.size + w_out.size), bytes_accessed=2 * (w_up.size + w_down.size + w_out.size), transcendentals=batch * vocab),
        name="layer",
    )(*partials, ln2_gain, ln2_bias, lnf_gain, lnf_bias, w_up, w_down, w_out)
    blocks = 8
    return pl.pallas_call(
        subtract_kernel,
        out_shape=(jax.ShapeDtypeStruct((batch, width), bf16), jax.ShapeDtypeStruct((batch, vocab), f32)),
        in_specs=[vmem, hbm, hbm],
        out_specs=(hbm, hbm),
        scratch_shapes=[pltpu.VMEM((batch, width), bf16), pltpu.VMEM((blocks, batch // blocks, vocab), f32), dma((2,)), dma((blocks,)), dma((blocks,))],
        compiler_params=pltpu.CompilerParams(vmem_limit_bytes=VMEM_LIMIT),
        cost_estimate=pl.CostEstimate(flops=batch * vocab, bytes_accessed=8 * batch * vocab, transcendentals=0),
        name="subtract",
    )(lse, hidden, logits)


def solution(mesh):
    row_spec = P('bs', None)
    cache_spec = P('bs', None, 'tp', None)
    col_split = P(None, 'tp')
    row_split = P('tp', None)
    in_specs = (row_spec, cache_spec, cache_spec, P('bs'), P(), P(), col_split, col_split, col_split, row_split, P(), P(), col_split, row_split, P(), P(), col_split)
    out_specs = (P('bs', 'tp'), cache_spec, cache_spec, row_spec)

    def local_step(new_hidden, cache_k, cache_v, lengths, ln1_gain, ln1_bias, w_q, w_k, w_v, w_o, ln2_gain, ln2_bias, w_up, w_down, lnf_gain, lnf_bias, w_out):
        partials, new_cache_k, new_cache_v = attend(new_hidden, cache_k, cache_v, lengths, ln1_gain, ln1_bias, w_q, w_k, w_v, w_o)
        out_hidden, log_probs = finish_layer(partials, new_hidden, ln2_gain, ln2_bias, lnf_gain, lnf_bias, w_up, w_down, w_out)
        return log_probs, new_cache_k, new_cache_v, out_hidden

    return jax.shard_map(local_step, mesh=mesh, in_specs=in_specs, out_specs=out_specs, check_vma=False)
```
